8 devices in a mesh: layer: 1 (over z), tensor: 8 (over y, x, core).
Axes of the slice: x: 2, y: 2, z: 1, core: 2. Of those that a mesh axis runs over, the one named last changes fastest.
Arguments:
- gradient: bfloat16 [1024, 8192], P('layer', 'tensor')
- left_stat: float32 [1024, 1024], P('layer')
- right_stat: float32 [8192, 8192], P(('layer', 'tensor'))
- left_root: bfloat16 [1024, 1024], P('layer')
- right_root: bfloat16 [8192, 8192], P(('layer', 'tensor'))
- second_moment: float32 [1024, 8192], P('layer', 'tensor')
Outputs:
- output 1: float32 [1024, 1024], P('layer')
- output 2: float32 [8192, 8192], P(('layer', 'tensor'))
- output 3: float32 [1024, 8192], P('layer', 'tensor')
- output 4: float32 [1024, 8192], P('layer', 'tensor')
All inputs are finite; a program needn't handle non-finite values.
Results may differ from the reference program's by a relative error of at most 0.001.
Values are sent between devices in bfloat16 or wider.
A program may use at most 1 GiB of HBM per device.

```python
import math
import jax
import jax.numpy as jnp

NUM_ROWS = 1024
NUM_COLS = 8192
EMA_DECAY = 0.9
ADAM_EPS = 1e-8


def stat_pair(basis_mat, spectrum, base_level):
    dim_size = basis_mat.shape[0]
    eye_mat = jnp.eye(dim_size, dtype=jnp.float32)
    stat_mat = base_level * (eye_mat + jnp.dot(basis_mat * spectrum, basis_mat.T))
    root_core = jnp.dot(basis_mat * ((1.0 + spectrum) ** -0.25 - 1.0), basis_mat.T)
    root_mat = base_level ** -0.25 * (eye_mat + 0.5 * (root_core + root_core.T))
    return stat_mat, root_mat.astype(jnp.bfloat16)


def setup_inputs(seed: int = 0, part: int = 0) -> dict:
    key_list = jax.random.split(jax.random.fold_in(jax.random.key(seed), part), 8)
    rank_dim = 32
    grad_scale = (NUM_ROWS * NUM_COLS) ** -0.25
    left_basis = jnp.linalg.qr(jax.random.normal(key_list[0], (NUM_ROWS, rank_dim), jnp.float32))[0]
    right_basis = jnp.linalg.qr(jax.random.normal(key_list[1], (NUM_COLS, rank_dim), jnp.float32))[0]
    core_mix = jax.random.normal(key_list[2], (rank_dim, rank_dim), jnp.float32)
    noise_part = jax.random.normal(key_list[3], (NUM_ROWS, NUM_COLS), jnp.float32)
    low_rank = jnp.dot(jnp.dot(left_basis, core_mix), right_basis.T)
    gradient = grad_scale * (low_rank * (math.sqrt(NUM_ROWS * NUM_COLS) / rank_dim) + noise_part)
    left_spec = jax.random.uniform(key_list[4], (rank_dim,), jnp.float32, 0.25, 4.0) * (NUM_ROWS / rank_dim)
    right_spec = jax.random.uniform(key_list[5], (rank_dim,), jnp.float32, 0.25, 4.0) * (NUM_COLS / rank_dim)
    left_stat, left_root = stat_pair(left_basis, left_spec, grad_scale ** 2 * NUM_COLS / 9.0)
    right_stat, right_root = stat_pair(right_basis, right_spec, grad_scale ** 2 * NUM_ROWS / 9.0)
    col_gain = jnp.exp(jnp.linspace(-2.3, 2.3, NUM_COLS, dtype=jnp.float32))[None, :]
    second_moment = grad_scale ** 2 * col_gain * jax.random.uniform(key_list[6], (NUM_ROWS, NUM_COLS), jnp.float32, 0.25, 4.0)
    return {
        'gradient': gradient.astype(jnp.bfloat16),
        'left_stat': left_stat,
        'right_stat': right_stat,
        'left_root': left_root,
        'right_root': right_root,
        'second_moment': second_moment,
    }


def reference(gradient, left_stat, right_stat, left_root, right_root, second_moment):
    left_new = EMA_DECAY * left_stat + (1.0 - EMA_DECAY) * jnp.dot(gradient, gradient.T, preferred_element_type=jnp.float32)
    right_new = EMA_DECAY * right_stat + (1.0 - EMA_DECAY) * jnp.dot(gradient.T, gradient, preferred_element_type=jnp.float32)
    precond = jnp.dot(gradient, right_root, preferred_element_type=jnp.float32).astype(jnp.bfloat16)
    direction = jnp.dot(left_root, precond, preferred_element_type=jnp.float32)
    grad_f32 = gradient.astype(jnp.float32)
    moment_new = EMA_DECAY * second_moment + (1.0 - EMA_DECAY) * grad_f32 * grad_f32
    adam_dir = grad_f32 / (jnp.sqrt(moment_new) + ADAM_EPS)
    norm_ratio = jnp.sqrt(jnp.sum(adam_dir * adam_dir) / jnp.sum(direction * direction))
    return (left_new, right_new, direction * norm_ratio, moment_new)
```

```python
import jax
import jax.numpy as jnp
from jax import lax
from jax.sharding import PartitionSpec as P

EMA_DECAY = 0.9
ADAM_EPS = 1e-8


def solution(mesh):
    col_spec = P('layer', 'tensor')
    rep_spec = P('layer', None)
    row_spec = P(('layer', 'tensor'), None)

    def local_step(grad_loc, left_stat, right_loc, left_root, root_loc, moment_loc):
        grad_full = lax.all_gather(grad_loc, 'tensor', axis=1, tiled=True)
        me = lax.axis_index('tensor')
        width = grad_loc.shape[1]
        left_sum = lax.dot_general(grad_loc, grad_loc, (((1,), (1,)), ((), ())), preferred_element_type=jnp.float32)
        for hop in range(1, 8):
            other = lax.rem(me + hop, 8)
            block = lax.dynamic_slice_in_dim(grad_full, other * width, width, 1)
            left_sum = left_sum + lax.dot_general(block, block, (((1,), (1,)), ((), ())), preferred_element_type=jnp.float32)
        left_new = EMA_DECAY * left_stat + (1.0 - EMA_DECAY) * left_sum
        right_prod = lax.dot_general(grad_loc, grad_full, (((0,), (0,)), ((), ())), preferred_element_type=jnp.float32)
        right_new = EMA_DECAY * right_loc + (1.0 - EMA_DECAY) * right_prod
        precond = lax.dot_general(grad_full, root_loc, (((1,), (1,)), ((), ())), preferred_element_type=jnp.float32).astype(jnp.bfloat16)
        direction = jnp.dot(left_root, precond, preferred_element_type=jnp.float32)
        grad_f32 = grad_loc.astype(jnp.float32)
        moment_new = EMA_DECAY * moment_loc + (1.0 - EMA_DECAY) * grad_f32 * grad_f32
        adam_dir = grad_f32 / (jnp.sqrt(moment_new) + ADAM_EPS)
        local_sq = jnp.stack([jnp.sum(adam_dir * adam_dir), jnp.sum(direction * direction)])
        total_sq = lax.psum(local_sq, 'tensor')
        return (left_new, right_new, direction * jnp.sqrt(total_sq[0] / total_sq[1]), moment_new)

    return jax.shard_map(local_step, mesh=mesh, in_specs=(col_spec, rep_spec, row_spec, rep_spec, row_spec, col_spec), out_specs=(rep_spec, row_spec, col_spec, col_spec), check_vma=False)
```

```python
import jax
import jax.numpy as jnp
from jax import lax
from jax.experimental import pallas as pl
from jax.experimental.pallas import tpu as pltpu
from jax.sharding import PartitionSpec as P

EMA_DECAY = 0.9
ADAM_EPS = 1e-8
N = 1024
CW = 128
GW = 512
TW = 256
NDEV = 8
ICI = 12
EARLY = 4
F32 = jnp.float32
BF16 = jnp.bfloat16

NT = (((1,), (1,)), ((), ()))
NN = (((1,), (0,)), ((), ()))


def dot(a, b, dims):
    return lax.dot_general(a, b, dims, preferred_element_type=F32)


def gather_kernel(g_hbm, l_hbm, r_hbm, lr_hbm, rr_hbm, v_hbm,
                  r0, r1, r2, r3, r4, r5, r6, r7, dd, ln, ratio,
                  gg, gt, rr, mine, sums,
                  load_sem, rload_sem, rr_sem, lr_sem,
                  own_s, own_r, x_s, x_r, y_s, y_r, p_s, p_r, n_s, n_r):
    rn = (r0, r1, r2, r3, r4, r5, r6, r7)
    me = lax.axis_index('tensor')
    core = lax.rem(me, 2)
    xpos = lax.rem(lax.div(me, 2), 2)
    ypos = lax.div(me, 4)
    mate = me + 1 - 2 * core
    xnb = me + 2 - 4 * xpos
    ynb = me + 4 - 8 * ypos
    diag = xnb + 4 - 8 * ypos
    mx = mate + 2 - 4 * xpos
    my = mate + 4 - 8 * ypos
    md = mx + 4 - 8 * ypos

    def col(dev, chunk):
        return pl.multiple_of(dev * N + chunk * CW, CW)

    blocks = (me, mate, xnb, ynb, mx, my, diag, md)

    def group(g, late=False):
        if isinstance(g, int) and g < 4:
            return [(g // 2, (g % 2) * 4 + j) for j in range(4)]
        i = g - 4
        if late:
            return [(6, i - 8), (6, i - 4), (7, i - 8), (7, i - 4)]
        return [(2, lax.rem(i + 4, 8)), (3, i), (4, lax.rem(i + 4, 8)), (5, i)]

    def lanes(j, w=CW):
        return pl.ds(j * w, w)

    own_loads = [pltpu.make_async_copy(g_hbm.at[:, h * GW:(h + 1) * GW], gg.at[h], load_sem.at[h]) for h in range(2)]
    v_load = pltpu.make_async_copy(v_hbm, dd, load_sem.at[2])
    half = pl.ds(pl.multiple_of(core * GW, GW), GW)
    l_load = pltpu.make_async_copy(l_hbm.at[half, :], ln.at[half, :], load_sem.at[3])
    for c in own_loads:
        c.start()

    r_loads = [pltpu.make_async_copy(r_hbm.at[:, pl.ds(pl.multiple_of(dev * N, N), N)], rn[k], rload_sem.at[k])
               for k, dev in enumerate(blocks)]

    def rr_loads(pieces, slot):
        return [pltpu.make_async_copy(rr_hbm.at[:, pl.ds(col(blocks[b], c), CW)], rr.at[slot, :, lanes(j)], rr_sem.at[slot, j])
                for j, (b, c) in enumerate(pieces)]

    barrier = pltpu.get_barrier_semaphore()
    others = [lax.rem(me + k, NDEV) for k in range(1, NDEV)]
    for o in others:
        pl.semaphore_signal(barrier, inc=1, device_id={'tensor': o})
    v_load.start()
    for c in rr_loads(group(0), 0):
        c.start()
    r_loads[0].start()
    l_load.start()
    r_loads[1].start()
    for c in own_loads:
        c.wait()
    pl.semaphore_wait(barrier, NDEV - 1)

    def own_send(h):
        return pltpu.make_async_remote_copy(gg.at[h], gg.at[2 + h], own_s.at[h], own_r.at[h], device_id={'tensor': mate})

    def x_copy(n, src):
        return pltpu.make_async_remote_copy(src, gg.at[4 + n, :, lanes(0)], x_s.at[n], x_r.at[n], device_id={'tensor': xnb})

    def y_copy(n, src):
        return pltpu.make_async_remote_copy(src, gg.at[4 + n, :, lanes(1)], y_s.at[n], y_r.at[n], device_id={'tensor': ynb})

    def own_chunk(c):
        return gg.at[lax.div(c, 4), :, pl.ds(pl.multiple_of(lax.rem(c, 4) * CW, CW), CW)]

    def send_own(n):
        x_copy(n, own_chunk(lax.rem(n + 4, 8))).start()
        y_copy(n, own_chunk(n)).start()

    def send_forward(j):
        x_copy(8 + j, gg.at[4 + j, :, lanes(1)]).start()
        y_copy(8 + j, gg.at[4 + j, :, lanes(0)]).start()

    def mate_copy(i):
        return pltpu.make_async_remote_copy(gg.at[4 + i, :, lanes(0, TW)], gg.at[4 + i, :, lanes(1, TW)],
                                            p_s.at[i], p_r.at[i], device_id={'tensor': mate})

    for n in range(EARLY):
        send_own(jnp.int32(n))
    for h in range(2):
        own_send(h).start()
    for c in r_loads[2:]:
        c.start()

    v_load.wait()

    def adam(k, total):
        rows = pl.ds(pl.multiple_of(k * 64, 64), 64)
        for h in range(2):
            grad = gg[h, rows, :].astype(F32)
            moment = EMA_DECAY * dd[rows, lanes(h, GW)] + (1.0 - EMA_DECAY) * grad * grad
            a = grad / (jnp.sqrt(moment) + ADAM_EPS)
            total = total + jnp.sum(a * a, axis=0, keepdims=True)
        return total

    adam_sum = jnp.sum(lax.fori_loop(0, N // 64, adam, jnp.zeros((1, GW), F32)))

    def transpose(k, _):
        rows = pl.ds(pl.multiple_of(k * CW, CW), CW)
        for h in range(2):
            gt[lanes(h, GW), rows] = gg[h, rows, :].T
        return 0

    lax.fori_loop(0, N // CW, transpose, 0)

    def x_part(g, slot, first, k0, kw):
        def tile(n, _):
            cols = pl.ds(pl.multiple_of(n * TW, TW), TW)
            part = dot(gg[g, :, pl.ds(k0, kw)], rr[slot, cols, pl.ds(k0, kw)], NT)
            dd[:, cols] = part if first else dd[:, cols] + part
            return 0
        lax.fori_loop(0, N // TW, tile, 0)

    def r_part(g, h, pieces):
        part = (1.0 - EMA_DECAY) * dot(gt[...], gg[g, :, lanes(h, TW)], NN)
        for j in range(2):
            b, c = pieces[2 * h + j]
            where = pl.ds(pl.multiple_of(c * CW, CW), CW)
            rn[b][:, where] = EMA_DECAY * rn[b][:, where] + part[:, j * CW:(j + 1) * CW]

    def l_part(g, rows):
        def tile(n, _):
            cols = pl.ds(pl.multiple_of(n * TW, TW), TW)
            part = dot(gg[g, rows, :], gg[g, cols, :], NT)
            ln[rows, cols] = ln[rows, cols] + (1.0 - EMA_DECAY) * part
            return 0
        lax.fori_loop(0, N // TW, tile, 0)

    l_load.wait()

    def decay(k, _):
        rows = pl.ds(pl.multiple_of(core * GW + k * 64, 64), 64)
        ln[rows, :] = EMA_DECAY * ln[rows, :]
        return 0

    lax.fori_loop(0, GW // 64, decay, 0)

    for g in range(4):
        slot = g % 2
        for c in rr_loads(group(g + 1), 1 - slot):
            c.start()
        cols = group(g)
        if g == 2:
            own_send(0).wait()
            r_loads[1].wait()
        if g == 3:
            own_send(1).wait()
        if g == 0:
            r_loads[0].wait()
        for c in rr_loads(cols, slot):
            c.wait()
        x_part(g, slot, g == 0, 0, GW)
        for h in range(2):
            r_part(g, h, cols)
        l_part(g, half)
    for c in r_loads[2:]:
        c.wait()

    def arrive(i):
        x_copy(i, gg.at[4 + i, :, lanes(0)]).wait_recv()
        y_copy(i, gg.at[4 + i, :, lanes(1)]).wait_recv()
        mate_copy(i).start()

    def step(i, issue, late, next_late):
        g = 4 + i
        slot = lax.rem(i, 2)
        cols = group(g, late)
        for c in rr_loads(group(g + 1, next_late), 1 - slot):
            c.start()
        arrive(i)
        issue(i)
        r_part(g, 0, cols)
        mate_copy(i).wait_recv()
        r_part(g, 1, cols)
        for c in rr_loads(cols, slot):
            c.wait()
        x_part(g, slot, False, 0, GW)
        l_part(g, half)

    def first_steps(i, _):
        step(i, lambda n: send_own(n + 4), False, False)
        return 0

    def next_steps(i, _):
        step(i, lambda n: send_forward(n - 4), False, False)
        return 0

    def last_steps(i, _):
        step(i, lambda n: None, True, True)
        return 0

    lax.fori_loop(0, 4, first_steps, 0)
    lax.fori_loop(4, 7, next_steps, 0)
    step(jnp.int32(7), lambda n: send_forward(n - 4), False, True)

    for n in range(8):
        x_copy(n, own_chunk(jnp.int32((n + 4) % 8))).wait_send()
        y_copy(n, own_chunk(jnp.int32(n))).wait_send()
    lr_loads = [pltpu.make_async_copy(lr_hbm.at[:, h * GW:(h + 1) * GW], gg.at[h], lr_sem.at[h]) for h in range(2)]
    for c in lr_loads:
        c.start()
    lax.fori_loop(8, 11, last_steps, 0)

    l_send = pltpu.make_async_remote_copy(ln.at[half, :], ln.at[half, :], own_s.at[2], own_r.at[2], device_id={'tensor': mate})
    l_send.start()

    last = ICI - 1
    g = 4 + last
    slot = last % 2
    cols = group(jnp.int32(g), True)
    arrive(last)
    for c in rr_loads(cols, slot):
        c.wait()
    x_part(g, slot, False, 0, TW)
    mate_copy(last).wait_recv()

    def x_last(n, _):
        for h in range(2):
            c = pl.ds(pl.multiple_of(n * TW + h * GW, TW), TW)
            part = dot(gg[g, :, lanes(1, TW)], rr[slot, c, lanes(1, TW)], NT)
            gg[2 + h, :, pl.ds(pl.multiple_of(n * TW, TW), TW)] = (dd[:, c] + part).astype(BF16)
        return 0

    lax.fori_loop(0, 2, x_last, 0)
    for c in lr_loads:
        c.wait()

    def d_tile(n, total):
        for h in range(2):
            src = pl.ds(pl.multiple_of(n * TW, TW), TW)
            c = pl.ds(pl.multiple_of(n * TW + h * GW, TW), TW)
            part = dot(gg[0], gg[2 + h, 0:GW, src], NN) + dot(gg[1], gg[2 + h, GW:N, src], NN)
            dd[:, c] = part
            total = total + jnp.sum(part * part, axis=0, keepdims=True)
        return total

    dir_sum = jnp.sum(lax.fori_loop(0, 2, d_tile, jnp.zeros((1, TW), F32)))
    mine[0] = jnp.full((8, CW), adam_sum, F32)
    mine[1] = jnp.full((8, CW), dir_sum, F32)
    r_part(g, 0, cols)

    def norm_copy(k, slot_of, to):
        return pltpu.make_async_remote_copy(mine, sums.at[slot_of], n_s.at[k], n_r.at[k], device_id={'tensor': to})

    for k in range(1, NDEV):
        norm_copy(NDEV - 1 - k, NDEV - 1 - k, lax.rem(me + k, NDEV)).start()
    r_part(g, 1, cols)
    l_send.wait()
    l_part(g, pl.ds(0, GW))
    l_part(g, pl.ds(GW, GW))
    for k in range(1, NDEV):
        norm_copy(k - 1, k - 1, lax.rem(me + k, NDEV)).wait_recv()

    a_all = mine[0]
    d_all = mine[1]
    for k in range(NDEV - 1):
        a_all = a_all + sums[k, 0]
        d_all = d_all + sums[k, 1]
    ratio[...] = jnp.sqrt(a_all / d_all)

    for k in range(1, NDEV):
        norm_copy(NDEV - 1 - k, NDEV - 1 - k, lax.rem(me + k, NDEV)).wait_send()
    for j in range(4):
        x_copy(8 + j, gg.at[4 + j, :, lanes(1)]).wait_send()
        y_copy(8 + j, gg.at[4 + j, :, lanes(0)]).wait_send()
    for i in range(ICI):
        mate_copy(i).wait_send()


def write_kernel(r0, r1, r2, r3, r4, r5, r6, r7, dd, ln, ratio, g_hbm, v_hbm, l_out, r_out, d_out, v_out,
                 vbuf, gbuf, dbuf, in_sem, out_sem):
    loads = [pltpu.make_async_copy(v_hbm, vbuf, in_sem.at[0]), pltpu.make_async_copy(g_hbm, gbuf, in_sem.at[1])]
    for c in loads:
        c.start()
    stores = []

    def store(src, dst):
        c = pltpu.make_async_copy(src, dst, out_sem.at[len(stores)])
        c.start()
        stores.append(c)

    me = lax.axis_index('tensor')
    xpos = lax.rem(lax.div(me, 2), 2)
    mate = me + 1 - 2 * lax.rem(me, 2)
    xhop, yhop = 2 - 4 * xpos, 4 - 8 * lax.div(me, 4)
    blocks = (me, mate, me + xhop, me + yhop, mate + xhop, mate + yhop, me + xhop + yhop, mate + xhop + yhop)
    for src, dev in zip((r0, r1, r2, r3, r4, r5, r6, r7), blocks):
        store(src, r_out.at[:, pl.ds(pl.multiple_of(dev * N, N), N)])
    store(ln, l_out)
    scale = ratio[0:1, 0:1]

    def scaled(k, _):
        rows = pl.ds(pl.multiple_of(k * 64, 64), 64)
        dbuf[rows, :] = dd[rows, :] * scale
        return 0

    lax.fori_loop(0, N // 64, scaled, 0)
    store(dbuf, d_out)
    for c in loads:
        c.wait()

    def moment(k, _):
        rows = pl.ds(pl.multiple_of(k * 64, 64), 64)
        grad = gbuf[rows, :].astype(F32)
        vbuf[rows, :] = EMA_DECAY * vbuf[rows, :] + (1.0 - EMA_DECAY) * grad * grad
        return 0

    lax.fori_loop(0, N // 64, moment, 0)
    store(vbuf, v_out)
    for c in stores:
        c.wait()


def solution(mesh):
    col_spec = P('layer', 'tensor')
    rep_spec = P('layer', None)
    row_spec = P(('layer', 'tensor'), None)
    hbm = pl.BlockSpec(memory_space=pl.ANY)
    vmem = pl.BlockSpec(memory_space=pltpu.VMEM)
    dma = pltpu.SemaphoreType.DMA

    def local_step(grad_loc, left_stat, right_loc, left_root, root_loc, moment_loc):
        mids = pl.pallas_call(
            gather_kernel,
            name='gather_compute',
            out_shape=(pltpu.VMEM((N, N), F32),) * (NDEV + 2) + (pltpu.VMEM((8, CW), F32),),
            in_specs=[hbm] * 6,
            out_specs=(vmem,) * (NDEV + 3),
            scratch_shapes=[
                pltpu.VMEM((16, N, GW), BF16),
                pltpu.VMEM((N, N), BF16),
                pltpu.VMEM((2, N, GW), BF16),
                pltpu.VMEM((2, 8, CW), F32),
                pltpu.VMEM((NDEV - 1, 2, 8, CW), F32),
                dma((4,)), dma((8,)), dma((2, 4)), dma((2,)),
                dma((3,)), dma((3,)), dma((ICI,)), dma((ICI,)), dma((ICI,)), dma((ICI,)),
                dma((ICI,)), dma((ICI,)), dma((NDEV - 1,)), dma((NDEV - 1,)),
            ],
            compiler_params=pltpu.CompilerParams(collective_id=0, has_side_effects=True, vmem_limit_bytes=VM1),
            cost_estimate=pl.CostEstimate(flops=46 * 2**30, bytes_accessed=60 * 2**20, transcendentals=2**20),
        )(grad_loc, left_stat, right_loc, left_root, root_loc, moment_loc)
        left_new, right_new, direction, moment_new = pl.pallas_call(
            write_kernel,
            name='write_results',
            out_shape=(jax.ShapeDtypeStruct((N, N), F32), jax.ShapeDtypeStruct((N, NDEV * N), F32),
                       jax.ShapeDtypeStruct((N, N), F32), jax.ShapeDtypeStruct((N, N), F32)),
            in_specs=[vmem] * (NDEV + 3) + [pl.BlockSpec(memory_space=pltpu.HBM)] * 2,
            out_specs=(hbm,) * 4,
            scratch_shapes=[pltpu.VMEM((N, N), F32), pltpu.VMEM((N, N), BF16), pltpu.VMEM((N, N), F32), dma((2,)), dma((16,))],
            compiler_params=pltpu.CompilerParams(vmem_limit_bytes=VM2),
        )(*(pltpu.with_memory_space_constraint(t, pltpu.VMEM) for t in mids), grad_loc, moment_loc)
        return left_new, right_new, direction, moment_new

    return jax.shard_map(local_step, mesh=mesh, in_specs=(col_spec, rep_spec, row_spec, rep_spec, row_spec, col_spec),
                         out_specs=(rep_spec, row_spec, col_spec, col_spec), check_vma=False)


VM1 = 23 * 2**20
VM2 = VM1
```

```python
import jax
import jax.numpy as jnp
from jax import lax
from jax.experimental import pallas as pl
from jax.experimental.pallas import tpu as pltpu
from jax.sharding import PartitionSpec as P

EMA_DECAY = 0.9
ADAM_EPS = 1e-8
N = 1024
CW = 128
GW = 512
TW = 256
NDEV = 8
ICI = 12
EARLY = 4
F32 = jnp.float32
BF16 = jnp.bfloat16

NT = (((1,), (1,)), ((), ()))
NN = (((1,), (0,)), ((), ()))


def dot(a, b, dims):
    return lax.dot_general(a, b, dims, preferred_element_type=F32)


def gather_kernel(g_hbm, l_hbm, r_hbm, lr_hbm, rr_hbm, v_hbm,
                  rn, dd, ln, ratio,
                  gg, gt, rr, mine, sums,
                  load_sem, rload_sem, rr_sem, lr_sem,
                  own_s, own_r, x_s, x_r, y_s, y_r, p_s, p_r, n_s, n_r):
    me = lax.axis_index('tensor')
    core = lax.rem(me, 2)
    xhop = 2 - 4 * lax.rem(lax.div(me, 2), 2)
    yhop = 4 - 8 * lax.div(me, 4)
    mate = me + 1 - 2 * core
    xnb = me + xhop
    ynb = me + yhop

    def device(b):
        q = b // 2
        return me + (b % 2) * (mate - me) + (q % 2) * xhop + (q // 2) * yhop

    def pieces(g):
        i = g - 4
        late = i // 8
        xc, yc = (i + 4 * (1 - late)) % 8, i - 4 * late
        bx, by = 2 + 4 * late, 4 + 2 * late
        return [(bx, xc), (by, yc), (bx + 1, xc), (by + 1, yc)]

    def local_pieces(g):
        return [(g // 2, (g % 2) * 4 + j) for j in range(4)]

    def lanes(j, w=CW):
        return pl.ds(j * w, w)

    own_loads = [pltpu.make_async_copy(g_hbm.at[:, h * GW:(h + 1) * GW], gg.at[h], load_sem.at[h]) for h in range(2)]
    v_load = pltpu.make_async_copy(v_hbm, dd, load_sem.at[2])
    half = pl.ds(pl.multiple_of(core * GW, GW), GW)
    l_load = pltpu.make_async_copy(l_hbm.at[half, :], ln.at[half, :], load_sem.at[3])
    for c in own_loads:
        c.start()

    r_loads = [pltpu.make_async_copy(r_hbm.at[:, pl.ds(pl.multiple_of(device(b) * N, N), N)], rn.at[b], rload_sem.at[b])
               for b in range(NDEV)]

    def rr_loads(where, slot):
        return [pltpu.make_async_copy(rr_hbm.at[:, pl.ds(pl.multiple_of(device(b) * N + c * CW, CW), CW)],
                                      rr.at[slot, :, lanes(j)], rr_sem.at[slot, j]) for j, (b, c) in enumerate(where)]

    barrier = pltpu.get_barrier_semaphore()
    for k in range(1, NDEV):
        pl.semaphore_signal(barrier, inc=1, device_id={'tensor': lax.rem(me + k, NDEV)})
    v_load.start()
    for c in rr_loads(local_pieces(0), 0):
        c.start()
    r_loads[0].start()
    l_load.start()
    r_loads[1].start()
    for c in own_loads:
        c.wait()
    pl.semaphore_wait(barrier, NDEV - 1)

    def own_send(h):
        return pltpu.make_async_remote_copy(gg.at[h], gg.at[2 + h], own_s.at[h], own_r.at[h], device_id={'tensor': mate})

    def x_copy(n, src):
        return pltpu.make_async_remote_copy(src, gg.at[4 + n, :, lanes(0)], x_s.at[n], x_r.at[n], device_id={'tensor': xnb})

    def y_copy(n, src):
        return pltpu.make_async_remote_copy(src, gg.at[4 + n, :, lanes(1)], y_s.at[n], y_r.at[n], device_id={'tensor': ynb})

    def own_chunk(c):
        return gg.at[c // 4, :, pl.ds(pl.multiple_of((c % 4) * CW, CW), CW)]

    def send_own(n):
        x_copy(n, own_chunk((n + 4) % 8)).start()
        y_copy(n, own_chunk(n)).start()

    def send_forward(j):
        x_copy(8 + j, gg.at[4 + j, :, lanes(1)]).start()
        y_copy(8 + j, gg.at[4 + j, :, lanes(0)]).start()

    def mate_copy(i):
        return pltpu.make_async_remote_copy(gg.at[4 + i, :, lanes(0, TW)], gg.at[4 + i, :, lanes(1, TW)],
                                            p_s.at[i], p_r.at[i], device_id={'tensor': mate})

    for n in range(EARLY):
        send_own(n)
    for h in range(2):
        own_send(h).start()
    for c in r_loads[2:]:
        c.start()

    v_load.wait()

    def adam(k, total):
        rows = pl.ds(pl.multiple_of(k * 64, 64), 64)
        for h in range(2):
            grad = gg[h, rows, :].astype(F32)
            moment = EMA_DECAY * dd[rows, lanes(h, GW)] + (1.0 - EMA_DECAY) * grad * grad
            a = grad / (jnp.sqrt(moment) + ADAM_EPS)
            dd[rows, lanes(h, GW)] = jnp.zeros((64, GW), F32)
            total = total + jnp.sum(a * a, axis=0, keepdims=True)
        return total

    adam_sum = jnp.sum(lax.fori_loop(0, N // 64, adam, jnp.zeros((1, GW), F32)))

    def transpose(k, _):
        rows = pl.ds(pl.multiple_of(k * CW, CW), CW)
        for h in range(2):
            gt[lanes(h, GW), rows] = gg[h, rows, :].T
        return 0

    lax.fori_loop(0, N // CW, transpose, 0)

    def x_part(g, slot):
        for n in range(N // TW):
            cols = lanes(n, TW)
            dd[:, cols] = dd[:, cols] + dot(gg[g], rr[slot, cols, :], NT)

    def r_part(g, h, where):
        part = (1.0 - EMA_DECAY) * dot(gt[...], gg[g, :, lanes(h, TW)], NN)
        for j in range(2):
            b, c = where[2 * h + j]
            cols = pl.ds(pl.multiple_of(c * CW, CW), CW)
            rn[b, :, cols] = EMA_DECAY * rn[b, :, cols] + part[:, j * CW:(j + 1) * CW]

    def l_part(g, rows):
        for n in range(N // TW):
            cols = lanes(n, TW)
            ln[rows, cols] = ln[rows, cols] + (1.0 - EMA_DECAY) * dot(gg[g, rows, :], gg[g, cols, :], NT)

    l_load.wait()

    def decay(k, _):
        rows = pl.ds(pl.multiple_of(core * GW + k * 64, 64), 64)
        ln[rows, :] = EMA_DECAY * ln[rows, :]
        return 0

    lax.fori_loop(0, GW // 64, decay, 0)
    r_loads[0].wait()

    def arrive(i):
        x_copy(i, gg.at[4 + i, :, lanes(0)]).wait_recv()
        y_copy(i, gg.at[4 + i, :, lanes(1)]).wait_recv()
        mate_copy(i).start()

    def local_step(g, _):
        slot = g % 2
        where = local_pieces(g)

        @pl.when(g < 3)
        def _():
            for c in rr_loads(local_pieces(g + 1), 1 - slot):
                c.start()

        @pl.when(g == 3)
        def _():
            for c in rr_loads(pieces(g + 1), 1 - slot):
                c.start()

        @pl.when(g >= 2)
        def _():
            own_send(g - 2).wait()

        @pl.when(g == 2)
        def _():
            r_loads[1].wait()

        for c in rr_loads(where, slot):
            c.wait()
        r_part(g, 0, where)
        r_part(g, 1, where)
        x_part(g, slot)
        l_part(g, half)
        return 0

    lax.fori_loop(0, 4, local_step, 0)
    for c in r_loads[2:]:
        c.wait()

    lr_loads = [pltpu.make_async_copy(lr_hbm.at[:, h * GW:(h + 1) * GW], gg.at[h], lr_sem.at[h]) for h in range(2)]

    def step(i, _):
        g = 4 + i
        slot = i % 2
        where = pieces(g)
        for c in rr_loads(pieces(g + 1), 1 - slot):
            c.start()
        arrive(i)

        @pl.when(i < 8 - EARLY)
        def _():
            send_own(i + EARLY)

        @pl.when((i >= 8 - EARLY) & (i < ICI - EARLY))
        def _():
            send_forward(i + EARLY - 8)

        @pl.when(i == 9)
        def _():
            for n in range(8):
                x_copy(n, own_chunk((n + 4) % 8)).wait_send()
                y_copy(n, own_chunk(n)).wait_send()
            for c in lr_loads:
                c.start()

        r_part(g, 0, where)
        mate_copy(i).wait_recv()
        for c in rr_loads(where, slot):
            c.wait()
        r_part(g, 1, where)
        x_part(g, slot)
        l_part(g, half)
        return 0

    last = ICI - 1
    lax.fori_loop(0, last, step, 0)

    l_send = pltpu.make_async_remote_copy(ln.at[half, :], ln.at[half, :], own_s.at[2], own_r.at[2], device_id={'tensor': mate})
    l_send.start()

    g = 4 + last
    slot = last % 2
    where = pieces(g)
    arrive(last)
    for c in rr_loads(where, slot):
        c.wait()
    for n in range(N // TW):
        cols = lanes(n, TW)
        dd[:, cols] = dd[:, cols] + dot(gg[g, :, lanes(0, TW)], rr[slot, cols, lanes(0, TW)], NT)
    mate_copy(last).wait_recv()
    for n in range(N // TW):
        cols = lanes(n, TW)
        part = dot(gg[g, :, lanes(1, TW)], rr[slot, cols, lanes(1, TW)], NT)
        gg[2 + n // 2, :, lanes(n % 2, TW)] = (dd[:, cols] + part).astype(BF16)
    for c in lr_loads:
        c.wait()
    total = jnp.zeros((1, TW), F32)
    for n in range(N // TW):
        src = lanes(n % 2, TW)
        part = dot(gg[0], gg[2 + n // 2, 0:GW, src], NN) + dot(gg[1], gg[2 + n // 2, GW:N, src], NN)
        dd[:, lanes(n, TW)] = part
        total = total + jnp.sum(part * part, axis=0, keepdims=True)
    mine[0] = jnp.full((8, CW), adam_sum, F32)
    mine[1] = jnp.full((8, CW), jnp.sum(total), F32)
    r_part(g, 0, where)

    def norm_copy(k, slot_of, to):
        return pltpu.make_async_remote_copy(mine, sums.at[slot_of], n_s.at[k], n_r.at[k], device_id={'tensor': to})

    for k in range(1, NDEV):
        norm_copy(NDEV - 1 - k, NDEV - 1 - k, lax.rem(me + k, NDEV)).start()
    r_part(g, 1, where)
    l_send.wait()
    l_part(g, pl.ds(0, N))
    for k in range(1, NDEV):
        norm_copy(k - 1, k - 1, lax.rem(me + k, NDEV)).wait_recv()

    a_all = mine[0]
    d_all = mine[1]
    for k in range(NDEV - 1):
        a_all = a_all + sums[k, 0]
        d_all = d_all + sums[k, 1]
    ratio[...] = jnp.sqrt(a_all / d_all)

    for k in range(1, NDEV):
        norm_copy(NDEV - 1 - k, NDEV - 1 - k, lax.rem(me + k, NDEV)).wait_send()
    for j in range(4):
        x_copy(8 + j, gg.at[4 + j, :, lanes(1)]).wait_send()
        y_copy(8 + j, gg.at[4 + j, :, lanes(0)]).wait_send()
    for i in range(ICI):
        mate_copy(i).wait_send()


def write_kernel(rn, dd, ln, ratio, g_hbm, v_hbm, l_out, r_out, d_out, v_out,
                 vbuf, gbuf, dbuf, in_sem, out_sem):
    loads = [pltpu.make_async_copy(v_hbm, vbuf, in_sem.at[0]), pltpu.make_async_copy(g_hbm, gbuf, in_sem.at[1])]
    for c in loads:
        c.start()
    stores = []

    def store(src, dst):
        c = pltpu.make_async_copy(src, dst, out_sem.at[len(stores)])
        c.start()
        stores.append(c)

    me = lax.axis_index('tensor')
    to_mate = 1 - 2 * lax.rem(me, 2)
    xhop, yhop = 2 - 4 * lax.rem(lax.div(me, 2), 2), 4 - 8 * lax.div(me, 4)
    for b in range(NDEV):
        dev = me + (b % 2) * to_mate + (b // 2 % 2) * xhop + (b // 4) * yhop
        store(rn.at[b], r_out.at[:, pl.ds(pl.multiple_of(dev * N, N), N)])
    store(ln, l_out)
    scale = ratio[0:1, 0:1]

    def scaled(k, _):
        rows = pl.ds(pl.multiple_of(k * 64, 64), 64)
        dbuf[rows, :] = dd[rows, :] * scale
        return 0

    lax.fori_loop(0, N // 64, scaled, 0)
    store(dbuf, d_out)
    for c in loads:
        c.wait()

    def moment(k, _):
        rows = pl.ds(pl.multiple_of(k * 64, 64), 64)
        grad = gbuf[rows, :].astype(F32)
        vbuf[rows, :] = EMA_DECAY * vbuf[rows, :] + (1.0 - EMA_DECAY) * grad * grad
        return 0

    lax.fori_loop(0, N // 64, moment, 0)
    store(vbuf, v_out)
    for c in stores:
        c.wait()


def solution(mesh):
    col_spec = P('layer', 'tensor')
    rep_spec = P('layer', None)
    row_spec = P(('layer', 'tensor'), None)
    hbm = pl.BlockSpec(memory_space=pl.ANY)
    vmem = pl.BlockSpec(memory_space=pltpu.VMEM)
    dma = pltpu.SemaphoreType.DMA

    def local_step(grad_loc, left_stat, right_loc, left_root, root_loc, moment_loc):
        mids = pl.pallas_call(
            gather_kernel,
            name='gather_compute',
            out_shape=(pltpu.VMEM((NDEV, N, N), F32), pltpu.VMEM((N, N), F32), pltpu.VMEM((N, N), F32), pltpu.VMEM((8, CW), F32)),
            in_specs=[hbm] * 6,
            out_specs=(vmem,) * 4,
            scratch_shapes=[
                pltpu.VMEM((16, N, GW), BF16),
                pltpu.VMEM((N, N), BF16),
                pltpu.VMEM((2, N, GW), BF16),
                pltpu.VMEM((2, 8, CW), F32),
                pltpu.VMEM((NDEV - 1, 2, 8, CW), F32),
                dma((4,)), dma((8,)), dma((2, 4)), dma((2,)),
                dma((3,)), dma((3,)), dma((ICI,)), dma((ICI,)), dma((ICI,)), dma((ICI,)),
                dma((ICI,)), dma((ICI,)), dma((NDEV - 1,)), dma((NDEV - 1,)),
            ],
            compiler_params=pltpu.CompilerParams(collective_id=0, has_side_effects=True, vmem_limit_bytes=VM1),
            cost_estimate=pl.CostEstimate(flops=46 * 2**30, bytes_accessed=60 * 2**20, transcendentals=2**20),
        )(grad_loc, left_stat, right_loc, left_root, root_loc, moment_loc)
        left_new, right_new, direction, moment_new = pl.pallas_call(
            write_kernel,
            name='write_results',
            out_shape=(jax.ShapeDtypeStruct((N, N), F32), jax.ShapeDtypeStruct((N, NDEV * N), F32),
                       jax.ShapeDtypeStruct((N, N), F32), jax.ShapeDtypeStruct((N, N), F32)),
            in_specs=[vmem] * 4 + [pl.BlockSpec(memory_space=pltpu.HBM)] * 2,
            out_specs=(hbm,) * 4,
            scratch_shapes=[pltpu.VMEM((N, N), F32), pltpu.VMEM((N, N), BF16), pltpu.VMEM((N, N), F32), dma((2,)), dma((16,))],
            compiler_params=pltpu.CompilerParams(vmem_limit_bytes=VM2),
        )(*(pltpu.with_memory_space_constraint(t, pltpu.VMEM) for t in mids), grad_loc, moment_loc)
        return left_new, right_new, direction, moment_new

    return jax.shard_map(local_step, mesh=mesh, in_specs=(col_spec, rep_spec, row_spec, rep_spec, row_spec, col_spec),
                         out_specs=(rep_spec, row_spec, col_spec, col_spec), check_vma=False)


VM1 = 23 * 2**20
VM2 = VM1
```

```python
import jax
import jax.numpy as jnp
from jax import lax
from jax.experimental import pallas as pl
from jax.experimental.pallas import tpu as pltpu
from jax.sharding import PartitionSpec as P

EMA_DECAY = 0.9
ADAM_EPS = 1e-8
N = 1024
CW = 128
GW = 512
TW = 256
NDEV = 8
ICI = 12
EARLY = 4
RING = 4
F32 = jnp.float32
BF16 = jnp.bfloat16

NT = (((1,), (1,)), ((), ()))
NN = (((1,), (0,)), ((), ()))


def dot(a, b, dims):
    return lax.dot_general(a, b, dims, preferred_element_type=F32)


def gather_kernel(g_hbm, l_hbm, r_hbm, lr_hbm, rr_hbm, v_hbm,
                  rn, dd, ln, vn, ratio,
                  gl, gi, gm, gt, rr, mine, sums,
                  load_sem, rload_sem, rr_sem, lr_sem,
                  own_s, own_r, x_s, x_r, y_s, y_r, p_s, p_r, n_s, n_r, credit):
    me = lax.axis_index('tensor')
    core = lax.rem(me, 2)
    xhop = 2 - 4 * lax.rem(lax.div(me, 2), 2)
    yhop = 4 - 8 * lax.div(me, 4)
    mate = me + 1 - 2 * core
    xnb = me + xhop
    ynb = me + yhop

    def device(b):
        q = b // 2
        return me + (b % 2) * (mate - me) + (q % 2) * xhop + (q // 2) * yhop

    def pieces(g):
        i = g - 4
        late = i // 8
        xc, yc = (i + 4 * (1 - late)) % 8, i - 4 * late
        bx, by = 2 + 4 * late, 4 + 2 * late
        return [(bx, xc), (by, yc), (bx + 1, xc), (by + 1, yc)]

    def local_pieces(g):
        return [(g // 2, (g % 2) * 4 + j) for j in range(4)]

    def lanes(j, w=CW):
        return pl.ds(j * w, w)

    own_loads = [pltpu.make_async_copy(g_hbm.at[:, h * GW:(h + 1) * GW], gl.at[h], load_sem.at[h]) for h in range(2)]
    v_load = pltpu.make_async_copy(v_hbm, vn, load_sem.at[2])
    half = pl.ds(pl.multiple_of(core * GW, GW), GW)
    l_load = pltpu.make_async_copy(l_hbm.at[half, :], ln.at[half, :], load_sem.at[3])
    for c in own_loads:
        c.start()

    r_loads = [pltpu.make_async_copy(r_hbm.at[:, pl.ds(pl.multiple_of(device(b) * N, N), N)], rn.at[b], rload_sem.at[b])
               for b in range(NDEV)]

    def rr_loads(where, slot):
        return [pltpu.make_async_copy(rr_hbm.at[:, pl.ds(pl.multiple_of(device(b) * N + c * CW, CW), CW)],
                                      rr.at[slot, :, lanes(j)], rr_sem.at[slot, j]) for j, (b, c) in enumerate(where)]

    barrier = pltpu.get_barrier_semaphore()
    for k in range(1, NDEV):
        pl.semaphore_signal(barrier, inc=1, device_id={'tensor': lax.rem(me + k, NDEV)})
    v_load.start()
    for c in rr_loads(local_pieces(0), 0):
        c.start()
    r_loads[0].start()
    l_load.start()
    r_loads[1].start()
    for c in own_loads:
        c.wait()
    pl.semaphore_wait(barrier, NDEV - 1)

    def own_send(h):
        return pltpu.make_async_remote_copy(gl.at[h], gl.at[2 + h], own_s.at[h], own_r.at[h], device_id={'tensor': mate})

    def x_copy(n, src):
        return pltpu.make_async_remote_copy(src, gi.at[n, :, lanes(0)], x_s.at[n], x_r.at[n], device_id={'tensor': xnb})

    def y_copy(n, src):
        return pltpu.make_async_remote_copy(src, gi.at[n, :, lanes(1)], y_s.at[n], y_r.at[n], device_id={'tensor': ynb})

    def own_chunk(c):
        return gl.at[c // 4, :, pl.ds(pl.multiple_of((c % 4) * CW, CW), CW)]

    def send_own(n):
        x_copy(n, own_chunk((n + 4) % 8)).start()
        y_copy(n, own_chunk(n)).start()

    def send_forward(j):
        x_copy(8 + j, gi.at[j, :, lanes(1)]).start()
        y_copy(8 + j, gi.at[j, :, lanes(0)]).start()

    def mate_copy(i):
        return pltpu.make_async_remote_copy(gi.at[i], gm.at[i % RING], p_s.at[i], p_r.at[i], device_id={'tensor': mate})

    for n in range(EARLY):
        send_own(n)
    for h in range(2):
        own_send(h).start()
    for c in r_loads[2:]:
        c.start()

    v_load.wait()

    def adam(k, total):
        rows = pl.ds(pl.multiple_of(k * 64, 64), 64)
        for h in range(2):
            grad = gl[h, rows, :].astype(F32)
            moment = EMA_DECAY * vn[rows, lanes(h, GW)] + (1.0 - EMA_DECAY) * grad * grad
            a = grad / (jnp.sqrt(moment) + ADAM_EPS)
            vn[rows, lanes(h, GW)] = moment
            dd[rows, lanes(h, GW)] = jnp.zeros((64, GW), F32)
            total = total + jnp.sum(a * a, axis=0, keepdims=True)
        return total

    adam_sum = jnp.sum(lax.fori_loop(0, N // 64, adam, jnp.zeros((1, GW), F32)))

    def transpose(k, _):
        rows = pl.ds(pl.multiple_of(k * CW, CW), CW)
        for h in range(2):
            gt[lanes(h, GW), rows] = gl[h, rows, :].T
        return 0

    lax.fori_loop(0, N // CW, transpose, 0)

    def x_part(halves, slot):
        for n in range(N // TW):
            cols = lanes(n, TW)
            part = sum(dot(a[...], rr[slot, cols, lanes(h, TW)], NT) for h, a in enumerate(halves))
            dd[:, cols] = dd[:, cols] + part

    def r_part(a, where):
        part = (1.0 - EMA_DECAY) * dot(gt[...], a[...], NN)
        for j, (b, c) in enumerate(where):
            cols = pl.ds(pl.multiple_of(c * CW, CW), CW)
            rn[b, :, cols] = EMA_DECAY * rn[b, :, cols] + part[:, j * CW:(j + 1) * CW]

    def l_part(halves, rows):
        for n in range(N // TW):
            cols = lanes(n, TW)
            part = sum(dot(a[rows, :], a[cols, :], NT) for a in halves)
            ln[rows, cols] = ln[rows, cols] + (1.0 - EMA_DECAY) * part

    l_load.wait()

    def decay(k, _):
        rows = pl.ds(pl.multiple_of(core * GW + k * 64, 64), 64)
        ln[rows, :] = EMA_DECAY * ln[rows, :]
        return 0

    lax.fori_loop(0, GW // 64, decay, 0)
    r_loads[0].wait()

    def arrive(i):
        x_copy(i, gi.at[i, :, lanes(0)]).wait_recv()
        y_copy(i, gi.at[i, :, lanes(1)]).wait_recv()
        if isinstance(i, int) and i < RING:
            mate_copy(i).start()
            return

        @pl.when(i >= RING)
        def _():
            pl.semaphore_wait(credit, 1)

        mate_copy(i).start()

    def issue(i):
        @pl.when(i < 8 - EARLY)
        def _():
            send_own(i + EARLY)

        @pl.when((i >= 8 - EARLY) & (i < ICI - EARLY))
        def _():
            send_forward(i + EARLY - 8)

    def local_step(g, _):
        slot = g % 2
        where = local_pieces(g)
        halves = [gl.at[g, :, lanes(h, TW)] for h in range(2)]

        @pl.when(g < 3)
        def _():
            for c in rr_loads(local_pieces(g + 1), 1 - slot):
                c.start()

        @pl.when(g == 3)
        def _():
            for c in rr_loads(pieces(4), 0):
                c.start()

        @pl.when(g >= 2)
        def _():
            own_send(g - 2).wait()

        @pl.when(g == 2)
        def _():
            r_loads[1].wait()

        for c in rr_loads(where, slot):
            c.wait()
        x_part(halves, slot)
        r_part(halves[0], where[:2])

        @pl.when(g == 3)
        def _():
            arrive(0)
            issue(0)
            for c in r_loads[2:]:
                c.wait()

        r_part(halves[1], where[2:])
        l_part(halves, half)
        return 0

    lax.fori_loop(0, 4, local_step, 0)

    lr_loads = [pltpu.make_async_copy(lr_hbm.at[:, h * GW:(h + 1) * GW], gl.at[h], lr_sem.at[h]) for h in range(2)]

    def step(i, _):
        slot = i % 2
        where = pieces(4 + i)
        halves = [gi.at[i], gm.at[i % RING]]
        for c in rr_loads(pieces(5 + i), 1 - slot):
            c.start()

        @pl.when(i == 9)
        def _():
            for n in range(8):
                x_copy(n, own_chunk((n + 4) % 8)).wait_send()
                y_copy(n, own_chunk(n)).wait_send()
            for c in lr_loads:
                c.start()

        mate_copy(i).wait_recv()
        for c in rr_loads(where, slot):
            c.wait()
        x_part(halves, slot)
        r_part(halves[0], where[:2])
        arrive(i + 1)
        issue(i + 1)
        r_part(halves[1], where[2:])
        l_part(halves, half)

        @pl.when(i < ICI - RING)
        def _():
            pl.semaphore_signal(credit, inc=1, device_id={'tensor': mate})

        return 0

    last = ICI - 1
    lax.fori_loop(0, last, step, 0)

    l_send = pltpu.make_async_remote_copy(ln.at[half, :], ln.at[half, :], own_s.at[2], own_r.at[2], device_id={'tensor': mate})
    l_send.start()

    slot = last % 2
    where = pieces(4 + last)
    halves = [gi.at[last], gm.at[last % RING]]
    for c in rr_loads(where, slot):
        c.wait()
    mate_copy(last).wait_recv()
    for n in range(N // TW):
        cols = lanes(n, TW)
        part = sum(dot(a[...], rr[slot, cols, lanes(h, TW)], NT) for h, a in enumerate(halves))
        gl[2 + n // 2, :, lanes(n % 2, TW)] = (dd[:, cols] + part).astype(BF16)
    for c in lr_loads:
        c.wait()
    total = jnp.zeros((1, TW), F32)
    for n in range(N // TW):
        src = lanes(n % 2, TW)
        part = dot(gl[0], gl[2 + n // 2, 0:GW, src], NN) + dot(gl[1], gl[2 + n // 2, GW:N, src], NN)
        dd[:, lanes(n, TW)] = part
        total = total + jnp.sum(part * part, axis=0, keepdims=True)
    mine[0] = jnp.full((8, CW), adam_sum, F32)
    mine[1] = jnp.full((8, CW), jnp.sum(total), F32)
    r_part(halves[0], where[:2])

    def norm_copy(k, slot_of, to):
        return pltpu.make_async_remote_copy(mine, sums.at[slot_of], n_s.at[k], n_r.at[k], device_id={'tensor': to})

    for k in range(1, NDEV):
        norm_copy(NDEV - 1 - k, NDEV - 1 - k, lax.rem(me + k, NDEV)).start()
    r_part(halves[1], where[2:])
    l_send.wait()
    l_part(halves, pl.ds(0, N))
    for k in range(1, NDEV):
        norm_copy(k - 1, k - 1, lax.rem(me + k, NDEV)).wait_recv()

    a_all = mine[0]
    d_all = mine[1]
    for k in range(NDEV - 1):
        a_all = a_all + sums[k, 0]
        d_all = d_all + sums[k, 1]
    ratio[...] = jnp.sqrt(a_all / d_all)

    for k in range(1, NDEV):
        norm_copy(NDEV - 1 - k, NDEV - 1 - k, lax.rem(me + k, NDEV)).wait_send()
    for j in range(4):
        x_copy(8 + j, gi.at[j, :, lanes(1)]).wait_send()
        y_copy(8 + j, gi.at[j, :, lanes(0)]).wait_send()
    for i in range(ICI):
        mate_copy(i).wait_send()


def write_kernel(rn, dd, ln, vn, ratio, l_out, r_out, d_out, v_out, dbuf, out_sem):
    stores = []

    def store(src, dst):
        c = pltpu.make_async_copy(src, dst, out_sem.at[len(stores)])
        c.start()
        stores.append(c)

    me = lax.axis_index('tensor')
    to_mate = 1 - 2 * lax.rem(me, 2)
    xhop, yhop = 2 - 4 * lax.rem(lax.div(me, 2), 2), 4 - 8 * lax.div(me, 4)
    for b in range(NDEV):
        dev = me + (b % 2) * to_mate + (b // 2 % 2) * xhop + (b // 4) * yhop
        store(rn.at[b], r_out.at[:, pl.ds(pl.multiple_of(dev * N, N), N)])
    store(ln, l_out)
    store(vn, v_out)
    scale = ratio[0:1, 0:1]

    def scaled(k, _):
        rows = pl.ds(pl.multiple_of(k * 64, 64), 64)
        dbuf[rows, :] = dd[rows, :] * scale
        return 0

    lax.fori_loop(0, N // 64, scaled, 0)
    store(dbuf, d_out)
    for c in stores:
        c.wait()


def solution(mesh):
    col_spec = P('layer', 'tensor')
    rep_spec = P('layer', None)
    row_spec = P(('layer', 'tensor'), None)
    hbm = pl.BlockSpec(memory_space=pl.ANY)
    vmem = pl.BlockSpec(memory_space=pltpu.VMEM)
    dma = pltpu.SemaphoreType.DMA

    def local_step(grad_loc, left_stat, right_loc, left_root, root_loc, moment_loc):
        mids = pl.pallas_call(
            gather_kernel,
            name='gather_compute',
            out_shape=(pltpu.VMEM((NDEV, N, N), F32), pltpu.VMEM((N, N), F32), pltpu.VMEM((N, N), F32), pltpu.VMEM((N, N), F32), pltpu.VMEM((8, CW), F32)),
            in_specs=[hbm] * 6,
            out_specs=(vmem,) * 5,
            scratch_shapes=[
                pltpu.VMEM((4, N, GW), BF16),
                pltpu.VMEM((ICI, N, TW), BF16),
                pltpu.VMEM((RING, N, TW), BF16),
                pltpu.VMEM((N, N), BF16),
                pltpu.VMEM((2, N, GW), BF16),
                pltpu.VMEM((2, 8, CW), F32),
                pltpu.VMEM((NDEV - 1, 2, 8, CW), F32),
                dma((4,)), dma((8,)), dma((2, 4)), dma((2,)),
                dma((3,)), dma((3,)), dma((ICI,)), dma((ICI,)), dma((ICI,)), dma((ICI,)),
                dma((ICI,)), dma((ICI,)), dma((NDEV - 1,)), dma((NDEV - 1,)), pltpu.SemaphoreType.REGULAR,
            ],
            compiler_params=pltpu.CompilerParams(collective_id=0, has_side_effects=True, vmem_limit_bytes=VM1),
            cost_estimate=pl.CostEstimate(flops=46 * 2**30, bytes_accessed=60 * 2**20, transcendentals=2**20),
        )(grad_loc, left_stat, right_loc, left_root, root_loc, moment_loc)
        left_new, right_new, direction, moment_new = pl.pallas_call(
            write_kernel,
            name='write_results',
            out_shape=(jax.ShapeDtypeStruct((N, N), F32), jax.ShapeDtypeStruct((N, NDEV * N), F32),
                       jax.ShapeDtypeStruct((N, N), F32), jax.ShapeDtypeStruct((N, N), F32)),
            in_specs=[vmem] * 5,
            out_specs=(hbm,) * 4,
            scratch_shapes=[pltpu.VMEM((N, N), F32), dma((16,))],
            compiler_params=pltpu.CompilerParams(vmem_limit_bytes=VM2),
        )(*(pltpu.with_memory_space_constraint(t, pltpu.VMEM) for t in mids))
        return left_new, right_new, direction, moment_new

    return jax.shard_map(local_step, mesh=mesh, in_specs=(col_spec, rep_spec, row_spec, rep_spec, row_spec, col_spec),
                         out_specs=(rep_spec, row_spec, col_spec, col_spec), check_vma=False)


VM1 = 19 * 2**20
VM2 = VM1
```

```python
import jax
import jax.numpy as jnp
from jax import lax
from jax.experimental import pallas as pl
from jax.experimental.pallas import tpu as pltpu
from jax.sharding import PartitionSpec as P

EMA_DECAY = 0.9
ADAM_EPS = 1e-8
N = 1024
CW = 128
GW = 512
TW = 256
NDEV = 8
ICI = 12
EARLY = 4
RING = 4
F32 = jnp.float32
BF16 = jnp.bfloat16

NT = (((1,), (1,)), ((), ()))
NN = (((1,), (0,)), ((), ()))


def dot(a, b, dims):
    return lax.dot_general(a, b, dims, preferred_element_type=F32)


def gather_kernel(g_hbm, l_hbm, r_hbm, lr_hbm, rr_hbm, v_hbm,
                  rn, dd, ln, vn, ratio, gi, gm, gt,
                  gl, rr, mine, sums,
                  load_sem, rload_sem, rr_sem, lr_sem,
                  own_s, own_r, x_s, x_r, y_s, y_r, p_s, p_r, n_s, n_r, credit):
    me = lax.axis_index('tensor')
    core = lax.rem(me, 2)
    xhop = 2 - 4 * lax.rem(lax.div(me, 2), 2)
    yhop = 4 - 8 * lax.div(me, 4)
    mate = me + 1 - 2 * core
    xnb = me + xhop
    ynb = me + yhop

    def device(b):
        q = b // 2
        return me + (b % 2) * (mate - me) + (q % 2) * xhop + (q // 2) * yhop

    def pieces(g):
        i = g - 4
        late = i // 8
        xc, yc = (i + 4 * (1 - late)) % 8, i - 4 * late
        bx, by = 2 + 4 * late, 4 + 2 * late
        return [(bx, xc), (by, yc), (bx + 1, xc), (by + 1, yc)]

    def local_pieces(g):
        return [(g // 2, (g % 2) * 4 + j) for j in range(4)]

    def lanes(j, w=CW):
        return pl.ds(j * w, w)

    own_loads = [pltpu.make_async_copy(g_hbm.at[:, h * GW:(h + 1) * GW], gl.at[h], load_sem.at[h]) for h in range(2)]
    v_load = pltpu.make_async_copy(v_hbm, vn, load_sem.at[2])
    half = pl.ds(pl.multiple_of(core * GW, GW), GW)
    l_load = pltpu.make_async_copy(l_hbm.at[half, :], ln.at[half, :], load_sem.at[3])
    for c in own_loads:
        c.start()

    r_loads = [pltpu.make_async_copy(r_hbm.at[:, pl.ds(pl.multiple_of(device(b) * N, N), N)], rn.at[b], rload_sem.at[b])
               for b in range(NDEV)]

    def rr_loads(where, slot):
        return [pltpu.make_async_copy(rr_hbm.at[:, pl.ds(pl.multiple_of(device(b) * N + c * CW, CW), CW)],
                                      rr.at[slot, :, lanes(j)], rr_sem.at[slot, j]) for j, (b, c) in enumerate(where)]

    barrier = pltpu.get_barrier_semaphore()
    for k in range(1, NDEV):
        pl.semaphore_signal(barrier, inc=1, device_id={'tensor': lax.rem(me + k, NDEV)})
    v_load.start()
    for c in rr_loads(local_pieces(0), 0):
        c.start()
    r_loads[0].start()
    l_load.start()
    r_loads[1].start()
    for c in own_loads:
        c.wait()
    pl.semaphore_wait(barrier, NDEV - 1)

    def own_send(h):
        return pltpu.make_async_remote_copy(gl.at[h], gl.at[2 + h], own_s.at[h], own_r.at[h], device_id={'tensor': mate})

    def x_copy(n, src):
        return pltpu.make_async_remote_copy(src, gi.at[n, :, lanes(0)], x_s.at[n], x_r.at[n], device_id={'tensor': xnb})

    def y_copy(n, src):
        return pltpu.make_async_remote_copy(src, gi.at[n, :, lanes(1)], y_s.at[n], y_r.at[n], device_id={'tensor': ynb})

    def own_chunk(c):
        return gl.at[c // 4, :, pl.ds(pl.multiple_of((c % 4) * CW, CW), CW)]

    def send_own(n):
        x_copy(n, own_chunk((n + 4) % 8)).start()
        y_copy(n, own_chunk(n)).start()

    def send_forward(j):
        x_copy(8 + j, gi.at[j, :, lanes(1)]).start()
        y_copy(8 + j, gi.at[j, :, lanes(0)]).start()

    def mate_copy(i):
        return pltpu.make_async_remote_copy(gi.at[i], gm.at[i % RING], p_s.at[i], p_r.at[i], device_id={'tensor': mate})

    for n in range(EARLY):
        send_own(n)
    for h in range(2):
        own_send(h).start()
    for c in r_loads[2:]:
        c.start()

    v_load.wait()

    def adam(k, total):
        rows = pl.ds(pl.multiple_of(k * 64, 64), 64)
        for h in range(2):
            grad = gl[h, rows, :].astype(F32)
            moment = EMA_DECAY * vn[rows, lanes(h, GW)] + (1.0 - EMA_DECAY) * grad * grad
            a = grad / (jnp.sqrt(moment) + ADAM_EPS)
            vn[rows, lanes(h, GW)] = moment
            dd[rows, lanes(h, GW)] = jnp.zeros((64, GW), F32)
            total = total + jnp.sum(a * a, axis=0, keepdims=True)
        return total

    adam_sum = jnp.sum(lax.fori_loop(0, N // 64, adam, jnp.zeros((1, GW), F32)))

    def transpose(k, _):
        rows = pl.ds(pl.multiple_of(k * CW, CW), CW)
        for h in range(2):
            gt[lanes(h, GW), rows] = gl[h, rows, :].T
        return 0

    lax.fori_loop(0, N // CW, transpose, 0)

    def x_part(halves, slot):
        for n in range(N // TW):
            cols = lanes(n, TW)
            part = sum(dot(a[...], rr[slot, cols, lanes(h, TW)], NT) for h, a in enumerate(halves))
            dd[:, cols] = dd[:, cols] + part

    def r_part(a, where):
        part = (1.0 - EMA_DECAY) * dot(gt[...], a[...], NN)
        for j, (b, c) in enumerate(where):
            cols = pl.ds(pl.multiple_of(c * CW, CW), CW)
            rn[b, :, cols] = EMA_DECAY * rn[b, :, cols] + part[:, j * CW:(j + 1) * CW]

    def l_part(halves, rows):
        for n in range(N // TW):
            cols = lanes(n, TW)
            part = sum(dot(a[rows, :], a[cols, :], NT) for a in halves)
            ln[rows, cols] = ln[rows, cols] + (1.0 - EMA_DECAY) * part

    l_load.wait()

    def decay(k, _):
        rows = pl.ds(pl.multiple_of(core * GW + k * 64, 64), 64)
        ln[rows, :] = EMA_DECAY * ln[rows, :]
        return 0

    lax.fori_loop(0, GW // 64, decay, 0)
    r_loads[0].wait()

    def arrive(i):
        x_copy(i, gi.at[i, :, lanes(0)]).wait_recv()
        y_copy(i, gi.at[i, :, lanes(1)]).wait_recv()
        if isinstance(i, int) and i < RING:
            mate_copy(i).start()
            return

        @pl.when(i >= RING)
        def _():
            pl.semaphore_wait(credit, 1)

        mate_copy(i).start()

    def issue(i):
        @pl.when(i < 8 - EARLY)
        def _():
            send_own(i + EARLY)

        @pl.when((i >= 8 - EARLY) & (i < ICI - EARLY))
        def _():
            send_forward(i + EARLY - 8)

    def local_step(g, _):
        slot = g % 2
        where = local_pieces(g)
        halves = [gl.at[g, :, lanes(h, TW)] for h in range(2)]

        @pl.when(g < 3)
        def _():
            for c in rr_loads(local_pieces(g + 1), 1 - slot):
                c.start()

        @pl.when(g == 3)
        def _():
            for c in rr_loads(pieces(4), 0):
                c.start()

        @pl.when(g >= 2)
        def _():
            own_send(g - 2).wait()

        @pl.when(g == 2)
        def _():
            r_loads[1].wait()

        for c in rr_loads(where, slot):
            c.wait()
        x_part(halves, slot)
        r_part(halves[0], where[:2])

        @pl.when(g == 3)
        def _():
            arrive(0)
            issue(0)
            for c in r_loads[2:]:
                c.wait()

        r_part(halves[1], where[2:])
        l_part(halves, half)
        return 0

    lax.fori_loop(0, 4, local_step, 0)

    lr_loads = [pltpu.make_async_copy(lr_hbm.at[:, h * GW:(h + 1) * GW], gl.at[h], lr_sem.at[h]) for h in range(2)]

    def step(i, _):
        slot = i % 2
        where = pieces(4 + i)
        halves = [gi.at[i], gm.at[i % RING]]
        for c in rr_loads(pieces(5 + i), 1 - slot):
            c.start()

        mate_copy(i).wait_recv()
        for c in rr_loads(where, slot):
            c.wait()
        x_part(halves, slot)
        r_part(halves[0], where[:2])
        arrive(i + 1)
        issue(i + 1)
        r_part(halves[1], where[2:])
        l_part(halves, half)
        pl.semaphore_signal(credit, inc=1, device_id={'tensor': mate})
        return 0

    lax.fori_loop(0, 8, step, 0)

    def late_step(i, _):
        slot = i % 2
        for c in rr_loads(pieces(5 + i), 1 - slot):
            c.start()

        @pl.when(i == 9)
        def _():
            for n in range(8):
                x_copy(n, own_chunk((n + 4) % 8)).wait_send()
                y_copy(n, own_chunk(n)).wait_send()
            for c in lr_loads:
                c.start()

        mate_copy(i).wait_recv()
        for c in rr_loads(pieces(4 + i), slot):
            c.wait()
        x_part([gi.at[i], gm.at[i % RING]], slot)
        arrive(i + 1)
        l_part([gi.at[i], gm.at[i % RING]], half)
        return 0

    last = ICI - 1
    lax.fori_loop(8, last, late_step, 0)

    l_send = pltpu.make_async_remote_copy(ln.at[half, :], ln.at[half, :], own_s.at[2], own_r.at[2], device_id={'tensor': mate})
    l_send.start()
    slot = last % 2
    for c in rr_loads(pieces(4 + last), slot):
        c.wait()
    x_part([gi.at[last]], slot)
    for c in lr_loads:
        c.wait()
    mate_copy(last).wait_recv()
    for n in range(N // TW):
        cols = lanes(n, TW)
        part = dot(gm[last % RING], rr[slot, cols, lanes(1, TW)], NT)
        gl[2 + n // 2, :, lanes(n % 2, TW)] = (dd[:, cols] + part).astype(BF16)
    total = jnp.zeros((1, TW), F32)
    for n in range(N // TW):
        src = lanes(n % 2, TW)
        part = dot(gl[0], gl[2 + n // 2, 0:GW, src], NN) + dot(gl[1], gl[2 + n // 2, GW:N, src], NN)
        dd[:, lanes(n, TW)] = part
        total = total + jnp.sum(part * part, axis=0, keepdims=True)
    mine[0] = jnp.full((8, CW), adam_sum, F32)
    mine[1] = jnp.full((8, CW), jnp.sum(total), F32)

    def norm_copy(k, slot_of, to):
        return pltpu.make_async_remote_copy(mine, sums.at[slot_of], n_s.at[k], n_r.at[k], device_id={'tensor': to})

    for k in range(1, NDEV):
        norm_copy(NDEV - 1 - k, NDEV - 1 - k, lax.rem(me + k, NDEV)).start()
    l_send.wait()
    for k in range(1, NDEV):
        norm_copy(k - 1, k - 1, lax.rem(me + k, NDEV)).wait_recv()

    a_all = mine[0]
    d_all = mine[1]
    for k in range(NDEV - 1):
        a_all = a_all + sums[k, 0]
        d_all = d_all + sums[k, 1]
    ratio[...] = jnp.sqrt(a_all / d_all)

    for k in range(1, NDEV):
        norm_copy(NDEV - 1 - k, NDEV - 1 - k, lax.rem(me + k, NDEV)).wait_send()
    for j in range(4):
        x_copy(8 + j, gi.at[j, :, lanes(1)]).wait_send()
        y_copy(8 + j, gi.at[j, :, lanes(0)]).wait_send()
    for i in range(ICI):
        mate_copy(i).wait_send()


def write_kernel(rn_in, dd_in, ln_in, vn, ratio, gi, gm, gt, l_out, r_out, d_out, v_out, rn, dd, ln, sem):
    me = lax.axis_index('tensor')
    to_mate = 1 - 2 * lax.rem(me, 2)
    xhop, yhop = 2 - 4 * lax.rem(lax.div(me, 2), 2), 4 - 8 * lax.div(me, 4)
    stores = []

    def store(src, dst):
        c = pltpu.make_async_copy(src, dst, sem.at[len(stores)])
        c.start()
        stores.append(c)

    def columns(b, c, w):
        dev = me + (b % 2) * to_mate + (b // 2 % 2) * xhop + (b // 4) * yhop
        return pl.ds(pl.multiple_of(dev * N + c * CW, CW), w)

    for b in range(6):
        store(rn.at[b], r_out.at[:, columns(b, 0, N)])
    store(vn, v_out)
    scale = ratio[0:1, 0:1]
    for n in range(N // TW):
        cols = pl.ds(n * TW, TW)
        dd[:, cols] = dd[:, cols] * scale
    store(dd, d_out)
    for b, slots in ((6, [gi.at[i] for i in range(8, ICI)]), (7, [gm.at[i % RING] for i in range(8, ICI)])):
        for c, a in enumerate(slots):
            part = (1.0 - EMA_DECAY) * dot(gt[...], a[...], NN)
            for j in range(2):
                cols = pl.ds((c + 4 * j) * CW, CW)
                rn[b, :, cols] = EMA_DECAY * rn[b, :, cols] + part[:, j * CW:(j + 1) * CW]
        store(rn.at[b], r_out.at[:, columns(b, 0, N)])
    halves = [gi.at[ICI - 1], gm.at[(ICI - 1) % RING]]
    for n in range(N // TW):
        cols = pl.ds(n * TW, TW)
        part = sum(dot(a[...], a[cols, :], NT) for a in halves)
        ln[:, cols] = ln[:, cols] + (1.0 - EMA_DECAY) * part
    store(ln, l_out)
    for c in stores:
        c.wait()


def solution(mesh):
    col_spec = P('layer', 'tensor')
    rep_spec = P('layer', None)
    row_spec = P(('layer', 'tensor'), None)
    hbm = pl.BlockSpec(memory_space=pl.ANY)
    vmem = pl.BlockSpec(memory_space=pltpu.VMEM)
    dma = pltpu.SemaphoreType.DMA

    def local_step(grad_loc, left_stat, right_loc, left_root, root_loc, moment_loc):
        mids = pl.pallas_call(
            gather_kernel,
            name='gather_compute',
            out_shape=(pltpu.VMEM((NDEV, N, N), F32), pltpu.VMEM((N, N), F32), pltpu.VMEM((N, N), F32), pltpu.VMEM((N, N), F32), pltpu.VMEM((8, CW), F32),
                       pltpu.VMEM((ICI, N, TW), BF16), pltpu.VMEM((RING, N, TW), BF16), pltpu.VMEM((N, N), BF16)),
            in_specs=[hbm] * 6,
            out_specs=(vmem,) * 8,
            scratch_shapes=[
                pltpu.VMEM((4, N, GW), BF16),
                pltpu.VMEM((2, N, GW), BF16),
                pltpu.VMEM((2, 8, CW), F32),
                pltpu.VMEM((NDEV - 1, 2, 8, CW), F32),
                dma((4,)), dma((8,)), dma((2, 4)), dma((2,)),
                dma((3,)), dma((3,)), dma((ICI,)), dma((ICI,)), dma((ICI,)), dma((ICI,)),
                dma((ICI,)), dma((ICI,)), dma((NDEV - 1,)), dma((NDEV - 1,)), pltpu.SemaphoreType.REGULAR,
            ],
            compiler_params=pltpu.CompilerParams(collective_id=0, has_side_effects=True, vmem_limit_bytes=VM1),
            cost_estimate=pl.CostEstimate(flops=46 * 2**30, bytes_accessed=60 * 2**20, transcendentals=2**20),
        )(grad_loc, left_stat, right_loc, left_root, root_loc, moment_loc)
        left_new, right_new, direction, moment_new, _, _, _ = pl.pallas_call(
            write_kernel,
            name='write_results',
            out_shape=(jax.ShapeDtypeStruct((N, N), F32), jax.ShapeDtypeStruct((N, NDEV * N), F32),
                       jax.ShapeDtypeStruct((N, N), F32), jax.ShapeDtypeStruct((N, N), F32),
                       pltpu.VMEM((NDEV, N, N), F32), pltpu.VMEM((N, N), F32), pltpu.VMEM((N, N), F32)),
            in_specs=[vmem] * 8,
            out_specs=(hbm,) * 4 + (vmem,) * 3,
            input_output_aliases={0: 4, 1: 5, 2: 6},
            scratch_shapes=[dma((11,))],
            compiler_params=pltpu.CompilerParams(vmem_limit_bytes=VM2),
        )(*(pltpu.with_memory_space_constraint(t, pltpu.VMEM) for t in mids))
        return left_new, right_new, direction, moment_new

    return jax.shard_map(local_step, mesh=mesh, in_specs=(col_spec, rep_spec, row_spec, rep_spec, row_spec, col_spec),
                         out_specs=(rep_spec, row_spec, col_spec, col_spec), check_vma=False)


VM1 = 9 * 2**20
VM2 = VM1
```

```python
import jax
import jax.numpy as jnp
from jax import lax
from jax.experimental import pallas as pl
from jax.experimental.pallas import tpu as pltpu
from jax.sharding import PartitionSpec as P

EMA_DECAY = 0.9
ADAM_EPS = 1e-8
N = 1024
CW = 128
GW = 512
TW = 256
NDEV = 8
ICI = 12
EARLY = 4
RING = 4
F32 = jnp.float32
BF16 = jnp.bfloat16

NT = (((1,), (1,)), ((), ()))
NN = (((1,), (0,)), ((), ()))


def dot(a, b, dims):
    return lax.dot_general(a, b, dims, preferred_element_type=F32)


def gather_kernel(g_hbm, l_hbm, r_hbm, lr_hbm, rr_hbm, v_hbm,
                  rn, dd, ln, vn, ratio, gi, gm, gt,
                  gl, rr, mine, sums,
                  load_sem, rload_sem, rr_sem, lr_sem,
                  own_s, own_r, x_s, x_r, y_s, y_r, p_s, p_r, n_s, n_r, credit):
    me = lax.axis_index('tensor')
    core = lax.rem(me, 2)
    xhop = 2 - 4 * lax.rem(lax.div(me, 2), 2)
    yhop = 4 - 8 * lax.div(me, 4)
    mate = me + 1 - 2 * core
    xnb = me + xhop
    ynb = me + yhop

    def device(b):
        q = b // 2
        return me + (b % 2) * (mate - me) + (q % 2) * xhop + (q // 2) * yhop

    def pieces(g):
        i = g - 4
        late = i // 8
        xc, yc = (i + 4 * (1 - late)) % 8, i - 4 * late
        bx, by = 2 + 4 * late, 4 + 2 * late
        return [(bx, xc), (by, yc), (bx + 1, xc), (by + 1, yc)]

    def local_pieces(g):
        return [(g // 2, (g % 2) * 4 + j) for j in range(4)]

    def lanes(j, w=CW):
        return pl.ds(j * w, w)

    own_loads = [pltpu.make_async_copy(g_hbm.at[:, h * GW:(h + 1) * GW], gl.at[h], load_sem.at[h]) for h in range(2)]
    v_load = pltpu.make_async_copy(v_hbm, vn, load_sem.at[2])
    half = pl.ds(pl.multiple_of(core * GW, GW), GW)
    l_load = pltpu.make_async_copy(l_hbm.at[half, :], ln.at[half, :], load_sem.at[3])
    for c in own_loads:
        c.start()

    r_loads = [pltpu.make_async_copy(r_hbm.at[:, pl.ds(pl.multiple_of(device(b) * N, N), N)], rn.at[b], rload_sem.at[b])
               for b in range(NDEV)]

    def rr_loads(where, slot):
        return [pltpu.make_async_copy(rr_hbm.at[:, pl.ds(pl.multiple_of(device(b) * N + c * CW, CW), CW)],
                                      rr.at[slot, :, lanes(j)], rr_sem.at[slot, j]) for j, (b, c) in enumerate(where)]

    barrier = pltpu.get_barrier_semaphore()
    for k in range(1, NDEV):
        pl.semaphore_signal(barrier, inc=1, device_id={'tensor': lax.rem(me + k, NDEV)})
    for c in rr_loads(local_pieces(0), 0):
        c.start()
    r_loads[0].start()
    for c in own_loads:
        c.wait()
    pl.semaphore_wait(barrier, NDEV - 1)

    def own_send(h):
        return pltpu.make_async_remote_copy(gl.at[h], gl.at[2 + h], own_s.at[h], own_r.at[h], device_id={'tensor': mate})

    def x_copy(n, src):
        return pltpu.make_async_remote_copy(src, gi.at[n, :, lanes(0)], x_s.at[n], x_r.at[n], device_id={'tensor': xnb})

    def y_copy(n, src):
        return pltpu.make_async_remote_copy(src, gi.at[n, :, lanes(1)], y_s.at[n], y_r.at[n], device_id={'tensor': ynb})

    def own_chunk(c):
        return gl.at[c // 4, :, pl.ds(pl.multiple_of((c % 4) * CW, CW), CW)]

    def send_own(n):
        x_copy(n, own_chunk((n + 4) % 8)).start()
        y_copy(n, own_chunk(n)).start()

    def send_forward(j):
        x_copy(8 + j, gi.at[j, :, lanes(1)]).start()
        y_copy(8 + j, gi.at[j, :, lanes(0)]).start()

    pair = pl.ds(ICI - 2, 2)
    row_half = [pl.ds(h * GW, GW) for h in range(2)]

    def x_pair(h):
        return pltpu.make_async_remote_copy(gi.at[pl.ds(2, 2), row_half[h], lanes(1)], gi.at[pair, row_half[h], lanes(0)],
                                            x_s.at[ICI - 2 + h], x_r.at[ICI - 2 + h], device_id={'tensor': xnb})

    def y_pair(h):
        return pltpu.make_async_remote_copy(gi.at[pl.ds(2, 2), row_half[h], lanes(0)], gi.at[pair, row_half[h], lanes(1)],
                                            y_s.at[ICI - 2 + h], y_r.at[ICI - 2 + h], device_id={'tensor': ynb})

    def mate_pair(h):
        return pltpu.make_async_remote_copy(gi.at[pair, row_half[h]], gm.at[pl.ds(RING - 2, 2), row_half[h]],
                                            p_s.at[ICI - 2 + h], p_r.at[ICI - 2 + h], device_id={'tensor': mate})

    def mate_copy(i):
        return pltpu.make_async_remote_copy(gi.at[i], gm.at[i % RING], p_s.at[i], p_r.at[i], device_id={'tensor': mate})

    for n in range(EARLY):
        send_own(n)
    for h in range(2):
        own_send(h).start()
    l_load.start()
    r_loads[1].start()

    def transpose(k, _):
        rows = pl.ds(pl.multiple_of(k * CW, CW), CW)
        for h in range(2):
            gt[lanes(h, GW), rows] = gl[h, rows, :].T
        dd[rows, :] = jnp.zeros((CW, N), F32)
        return 0

    lax.fori_loop(0, N // CW, transpose, 0)

    def x_part(halves, slot):
        for n in range(N // TW):
            cols = lanes(n, TW)
            part = sum(dot(a[...], rr[slot, cols, lanes(h, TW)], NT) for h, a in enumerate(halves))
            dd[:, cols] = dd[:, cols] + part

    def r_part(a, where):
        part = (1.0 - EMA_DECAY) * dot(gt[...], a[...], NN)
        for j, (b, c) in enumerate(where):
            cols = pl.ds(pl.multiple_of(c * CW, CW), CW)
            rn[b, :, cols] = EMA_DECAY * rn[b, :, cols] + part[:, j * CW:(j + 1) * CW]

    def l_part(halves, rows):
        for n in range(N // TW):
            cols = lanes(n, TW)
            part = sum(dot(a[rows, :], a[cols, :], NT) for a in halves)
            ln[rows, cols] = ln[rows, cols] + (1.0 - EMA_DECAY) * part

    l_load.wait()

    def decay(k, _):
        rows = pl.ds(pl.multiple_of(core * GW + k * 64, 64), 64)
        ln[rows, :] = EMA_DECAY * ln[rows, :]
        return 0

    lax.fori_loop(0, GW // 64, decay, 0)
    r_loads[0].wait()

    def arrive(i):
        x_copy(i, gi.at[i, :, lanes(0)]).wait_recv()
        y_copy(i, gi.at[i, :, lanes(1)]).wait_recv()
        if isinstance(i, int) and i < RING:
            mate_copy(i).start()
            return

        @pl.when(i >= RING)
        def _():
            pl.semaphore_wait(credit, 1)

        mate_copy(i).start()

    def arrive_pair(h):
        x_pair(h).wait_recv()
        y_pair(h).wait_recv()
        mate_pair(h).start()

    def issue(i):
        @pl.when(i < 8 - EARLY)
        def _():
            send_own(i + EARLY)

        @pl.when((i >= 8 - EARLY) & (i < ICI - 2 - EARLY))
        def _():
            send_forward(i + EARLY - 8)

        for h in range(2):
            @pl.when(i == ICI - 2 - EARLY + h)
            def _():
                x_pair(h).start()
                y_pair(h).start()

    def local_step(g, _):
        slot = g % 2
        where = local_pieces(g)
        halves = [gl.at[g, :, lanes(h, TW)] for h in range(2)]

        @pl.when(g < 3)
        def _():
            for c in rr_loads(local_pieces(g + 1), 1 - slot):
                c.start()

        @pl.when(g == 3)
        def _():
            for c in rr_loads(pieces(4), 0):
                c.start()

        @pl.when(g >= 2)
        def _():
            own_send(g - 2).wait()

        @pl.when(g == 1)
        def _():
            for c in r_loads[2:4]:
                c.start()

        @pl.when(g == 2)
        def _():
            r_loads[1].wait()
            for c in r_loads[4:6]:
                c.start()

        for c in rr_loads(where, slot):
            c.wait()
        x_part(halves, slot)
        r_part(halves[0], where[:2])

        @pl.when(g == 3)
        def _():
            arrive(0)
            issue(0)
            for c in r_loads[2:6]:
                c.wait()

        r_part(halves[1], where[2:])
        l_part(halves, half)
        return 0

    lax.fori_loop(0, 4, local_step, 0)
    v_load.start()
    r_loads[6].start()

    lr_loads = [pltpu.make_async_copy(lr_hbm.at[:, h * GW:(h + 1) * GW], gl.at[h], lr_sem.at[h]) for h in range(2)]

    def step(i, _):
        slot = i % 2
        where = pieces(4 + i)
        halves = [gi.at[i], gm.at[i % RING]]
        for c in rr_loads(pieces(5 + i), 1 - slot):
            c.start()

        mate_copy(i).wait_recv()
        for c in rr_loads(where, slot):
            c.wait()
        x_part(halves, slot)
        r_part(halves[0], where[:2])
        arrive(i + 1)
        issue(i + 1)
        r_part(halves[1], where[2:])
        l_part(halves, half)
        pl.semaphore_signal(credit, inc=1, device_id={'tensor': mate})
        return 0

    lax.fori_loop(0, 8, step, 0)

    def late_step(i, slot):
        for c in rr_loads(pieces(5 + i), 1 - slot):
            c.start()
        mate_copy(i).wait_recv()
        for c in rr_loads(pieces(4 + i), slot):
            c.wait()
        x_part([gi.at[i], gm.at[i % RING]], slot)

    late_step(8, 0)

    v_load.wait()

    def adam(k, total):
        rows = pl.ds(pl.multiple_of(k * 64, 64), 64)
        for h in range(2):
            grad = gl[h, rows, :].astype(F32)
            moment = EMA_DECAY * vn[rows, lanes(h, GW)] + (1.0 - EMA_DECAY) * grad * grad
            a = grad / (jnp.sqrt(moment) + ADAM_EPS)
            vn[rows, lanes(h, GW)] = moment
            total = total + jnp.sum(a * a, axis=0, keepdims=True)
        return total

    adam_sum = jnp.sum(lax.fori_loop(0, N // 64, adam, jnp.zeros((1, GW), F32)))

    arrive(jnp.int32(9))
    l_part([gi.at[8], gm.at[0]], half)
    for n in range(8):
        x_copy(n, own_chunk((n + 4) % 8)).wait_send()
        y_copy(n, own_chunk(n)).wait_send()
    for c in lr_loads:
        c.start()
    late_step(9, 1)
    for c in rr_loads(pieces(15), 1):
        c.start()
    pl.semaphore_wait(credit, 2)
    arrive_pair(0)
    l_part([gi.at[9], gm.at[1]], half)

    l_send = pltpu.make_async_remote_copy(ln.at[half, :], ln.at[half, :], own_s.at[2], own_r.at[2], device_id={'tensor': mate})
    l_send.start()

    for slot in range(2):
        for c in rr_loads(pieces(14 + slot), slot):
            c.wait()
    for c in lr_loads:
        c.wait()
    share = rn.at[NDEV - 1]

    def x_rows(rows, mine_too, mates_too, done):
        for n in range(N // TW):
            cols = lanes(n, TW)
            value = dd[rows, cols]
            part = None
            for k in range(2):
                for take, a, at in ((mine_too, gi.at[ICI - 2 + k], 0), (mates_too, gm.at[RING - 2 + k], 1)):
                    if take:
                        term = dot(a[rows, :], rr[k, cols, lanes(at, TW)], NT)
                        part = term if part is None else part + term
            if done:
                gl[2 + n // 2, rows, lanes(n % 2, TW)] = (value + part).astype(BF16)
            else:
                dd[rows, cols] = value + part

    mate_pair(0).wait_recv()
    x_rows(row_half[0], True, True, True)
    for n in range(N // TW):
        share[:, lanes(n, TW)] = dot(gl[0], gl[2 + n // 2, row_half[0], lanes(n % 2, TW)], NN)
    arrive_pair(1)
    x_rows(row_half[1], True, False, False)
    mate_pair(1).wait_recv()
    x_rows(row_half[1], False, True, True)
    total = jnp.zeros((1, TW), F32)
    for n in range(N // TW):
        cols = lanes(n, TW)
        part = share[:, cols] + dot(gl[1], gl[2 + n // 2, row_half[1], lanes(n % 2, TW)], NN)
        dd[:, cols] = part
        total = total + jnp.sum(part * part, axis=0, keepdims=True)
    r_loads[NDEV - 1].start()
    mine[0] = jnp.full((8, CW), adam_sum, F32)
    mine[1] = jnp.full((8, CW), jnp.sum(total), F32)

    def norm_copy(k, slot_of, to):
        return pltpu.make_async_remote_copy(mine, sums.at[slot_of], n_s.at[k], n_r.at[k], device_id={'tensor': to})

    for k in range(1, NDEV):
        norm_copy(NDEV - 1 - k, NDEV - 1 - k, lax.rem(me + k, NDEV)).start()
    l_send.wait()
    for k in range(1, NDEV):
        norm_copy(k - 1, k - 1, lax.rem(me + k, NDEV)).wait_recv()

    a_all = mine[0]
    d_all = mine[1]
    for k in range(NDEV - 1):
        a_all = a_all + sums[k, 0]
        d_all = d_all + sums[k, 1]
    ratio[...] = jnp.sqrt(a_all / d_all)

    for k in range(1, NDEV):
        norm_copy(NDEV - 1 - k, NDEV - 1 - k, lax.rem(me + k, NDEV)).wait_send()
    for j in range(2):
        x_copy(8 + j, gi.at[j, :, lanes(1)]).wait_send()
        y_copy(8 + j, gi.at[j, :, lanes(0)]).wait_send()
        x_pair(j).wait_send()
        y_pair(j).wait_send()
        mate_pair(j).wait_send()
    for i in range(ICI - 2):
        mate_copy(i).wait_send()
    for c in r_loads[6:]:
        c.wait()


def write_kernel(rn_in, dd_in, ln_in, vn, ratio, gi, gm, gt, l_out, r_out, d_out, v_out, rn, dd, ln, sem):
    me = lax.axis_index('tensor')
    to_mate = 1 - 2 * lax.rem(me, 2)
    xhop, yhop = 2 - 4 * lax.rem(lax.div(me, 2), 2), 4 - 8 * lax.div(me, 4)
    stores = []

    def store(src, dst):
        c = pltpu.make_async_copy(src, dst, sem.at[len(stores)])
        c.start()
        stores.append(c)

    def columns(b, c, w):
        dev = me + (b % 2) * to_mate + (b // 2 % 2) * xhop + (b // 4) * yhop
        return pl.ds(pl.multiple_of(dev * N + c * CW, CW), w)

    for b in range(6):
        store(rn_in.at[b], r_out.at[:, columns(b, 0, N)])
    store(vn, v_out)
    scale = ratio[0:1, 0:1]
    for n in range(N // TW):
        cols = pl.ds(n * TW, TW)
        dd[:, cols] = dd_in[:, cols] * scale
    store(dd, d_out)
    for b, slots in ((6, [gi.at[i] for i in range(8, ICI)]), (7, [gm.at[i % RING] for i in range(8, ICI)])):
        for c, a in enumerate(slots):
            part = (1.0 - EMA_DECAY) * dot(gt[...], a[...], NN)
            for j in range(2):
                cols = pl.ds((c + 4 * j) * CW, CW)
                rn[b, :, cols] = EMA_DECAY * rn_in[b, :, cols] + part[:, j * CW:(j + 1) * CW]
        store(rn.at[b], r_out.at[:, columns(b, 0, N)])
    halves = [gi.at[ICI - 2], gi.at[ICI - 1], gm.at[RING - 2], gm.at[RING - 1]]
    for n in range(N // TW):
        cols = pl.ds(n * TW, TW)
        part = sum(dot(a[...], a[cols, :], NT) for a in halves)
        ln[:, cols] = ln_in[:, cols] + (1.0 - EMA_DECAY) * part
    store(ln, l_out)
    for c in stores:
        c.wait()


def solution(mesh):
    col_spec = P('layer', 'tensor')
    rep_spec = P('layer', None)
    row_spec = P(('layer', 'tensor'), None)
    hbm = pl.BlockSpec(memory_space=pl.ANY)
    vmem = pl.BlockSpec(memory_space=pltpu.VMEM)
    dma = pltpu.SemaphoreType.DMA

    def local_step(grad_loc, left_stat, right_loc, left_root, root_loc, moment_loc):
        mids = pl.pallas_call(
            gather_kernel,
            name='gather_compute',
            out_shape=(pltpu.VMEM((NDEV, N, N), F32), pltpu.VMEM((N, N), F32), pltpu.VMEM((N, N), F32), pltpu.VMEM((N, N), F32), pltpu.VMEM((8, CW), F32),
                       pltpu.VMEM((ICI, N, TW), BF16), pltpu.VMEM((RING, N, TW), BF16), pltpu.VMEM((N, N), BF16)),
            in_specs=[hbm] * 6,
            out_specs=(vmem,) * 8,
            scratch_shapes=[
                pltpu.VMEM((4, N, GW), BF16),
                pltpu.VMEM((2, N, GW), BF16),
                pltpu.VMEM((2, 8, CW), F32),
                pltpu.VMEM((NDEV - 1, 2, 8, CW), F32),
                dma((4,)), dma((8,)), dma((2, 4)), dma((2,)),
                dma((3,)), dma((3,)), dma((ICI,)), dma((ICI,)), dma((ICI,)), dma((ICI,)),
                dma((ICI,)), dma((ICI,)), dma((NDEV - 1,)), dma((NDEV - 1,)), pltpu.SemaphoreType.REGULAR,
            ],
            compiler_params=pltpu.CompilerParams(collective_id=0, has_side_effects=True, vmem_limit_bytes=VM1),
            cost_estimate=pl.CostEstimate(flops=46 * 2**30, bytes_accessed=60 * 2**20, transcendentals=2**20),
        )(grad_loc, left_stat, right_loc, left_root, root_loc, moment_loc)
        left_new, right_new, direction, moment_new, _, _, _ = pl.pallas_call(
            write_kernel,
            name='write_results',
            out_shape=(jax.ShapeDtypeStruct((N, N), F32), jax.ShapeDtypeStruct((N, NDEV * N), F32),
                       jax.ShapeDtypeStruct((N, N), F32), jax.ShapeDtypeStruct((N, N), F32),
                       pltpu.VMEM((NDEV, N, N), F32), pltpu.VMEM((N, N), F32), pltpu.VMEM((N, N), F32)),
            in_specs=[vmem] * 8,
            out_specs=(hbm,) * 4 + (vmem,) * 3,
            input_output_aliases={0: 4, 1: 5, 2: 6},
            scratch_shapes=[dma((11,))],
            compiler_params=pltpu.CompilerParams(vmem_limit_bytes=VM2),
        )(*(pltpu.with_memory_space_constraint(t, pltpu.VMEM) for t in mids))
        return left_new, right_new, direction, moment_new

    return jax.shard_map(local_step, mesh=mesh, in_specs=(col_spec, rep_spec, row_spec, rep_spec, row_spec, col_spec),
                         out_specs=(rep_spec, row_spec, col_spec, col_spec), check_vma=False)


VM1 = 79 * 2**17
VM2 = VM1
```

```python
import jax
import jax.numpy as jnp
from jax import lax
from jax.experimental import pallas as pl
from jax.experimental.pallas import tpu as pltpu
from jax.sharding import PartitionSpec as P

EMA_DECAY = 0.9
ADAM_EPS = 1e-8
N = 1024
CW = 128
GW = 512
TW = 256
NDEV = 8
ICI = 12
EARLY = 4
RING = 4
F32 = jnp.float32
BF16 = jnp.bfloat16

NT = (((1,), (1,)), ((), ()))
NN = (((1,), (0,)), ((), ()))


def dot(a, b, dims):
    return lax.dot_general(a, b, dims, preferred_element_type=F32)


def gather_kernel(g_hbm, l_hbm, r_hbm, lr_hbm, rr_hbm, v_hbm,
                  rn, dd, ln, vn, ratio, gi, gm, gt,
                  gl, rr, mine, sums,
                  load_sem, rload_sem, rr_sem, lr_sem,
                  own_s, own_r, x_s, x_r, y_s, y_r, p_s, p_r, n_s, n_r, credit):
    me = lax.axis_index('tensor')
    core = lax.rem(me, 2)
    xhop = 2 - 4 * lax.rem(lax.div(me, 2), 2)
    yhop = 4 - 8 * lax.div(me, 4)
    mate = me + 1 - 2 * core
    xnb = me + xhop
    ynb = me + yhop

    def device(b):
        q = b // 2
        return me + (b % 2) * (mate - me) + (q % 2) * xhop + (q // 2) * yhop

    def pieces(g):
        i = g - 4
        late = i // 8
        xc, yc = (i + 4 * (1 - late)) % 8, i - 4 * late
        bx, by = 2 + 4 * late, 4 + 2 * late
        return [(bx, xc), (by, yc), (bx + 1, xc), (by + 1, yc)]

    def local_pieces(g):
        return [(g // 2, (g % 2) * 4 + j) for j in range(4)]

    def lanes(j, w=CW):
        return pl.ds(j * w, w)

    own_loads = [pltpu.make_async_copy(g_hbm.at[:, h * GW:(h + 1) * GW], gl.at[h], load_sem.at[h]) for h in range(2)]
    v_load = pltpu.make_async_copy(v_hbm, vn, load_sem.at[2])
    half = pl.ds(pl.multiple_of(core * GW, GW), GW)
    l_load = pltpu.make_async_copy(l_hbm.at[half, :], ln.at[half, :], load_sem.at[3])
    for c in own_loads:
        c.start()

    r_loads = [pltpu.make_async_copy(r_hbm.at[:, pl.ds(pl.multiple_of(device(b) * N, N), N)], rn.at[b], rload_sem.at[b])
               for b in range(NDEV)]

    def rr_loads(where, slot):
        return [pltpu.make_async_copy(rr_hbm.at[:, pl.ds(pl.multiple_of(device(b) * N + c * CW, CW), CW)],
                                      rr.at[slot, :, lanes(j)], rr_sem.at[slot, j]) for j, (b, c) in enumerate(where)]

    barrier = pltpu.get_barrier_semaphore()
    for k in range(1, NDEV):
        pl.semaphore_signal(barrier, inc=1, device_id={'tensor': lax.rem(me + k, NDEV)})
    for c in rr_loads(local_pieces(0), 0):
        c.start()
    r_loads[0].start()
    for c in own_loads:
        c.wait()
    pl.semaphore_wait(barrier, NDEV - 1)

    def own_send(h):
        return pltpu.make_async_remote_copy(gl.at[h], gl.at[2 + h], own_s.at[h], own_r.at[h], device_id={'tensor': mate})

    def x_copy(n, src):
        return pltpu.make_async_remote_copy(src, gi.at[n, :, lanes(0)], x_s.at[n], x_r.at[n], device_id={'tensor': xnb})

    def y_copy(n, src):
        return pltpu.make_async_remote_copy(src, gi.at[n, :, lanes(1)], y_s.at[n], y_r.at[n], device_id={'tensor': ynb})

    def own_chunk(c):
        return gl.at[c // 4, :, pl.ds(pl.multiple_of((c % 4) * CW, CW), CW)]

    def send_own(n):
        x_copy(n, own_chunk((n + 4) % 8)).start()
        y_copy(n, own_chunk(n)).start()

    def send_forward(j):
        x_copy(8 + j, gi.at[j, :, lanes(1)]).start()
        y_copy(8 + j, gi.at[j, :, lanes(0)]).start()

    pair = pl.ds(ICI - 2, 2)
    row_half = [pl.ds(h * GW, GW) for h in range(2)]

    def x_pair(h):
        return pltpu.make_async_remote_copy(gi.at[pl.ds(2, 2), row_half[h], lanes(1)], gi.at[pair, row_half[h], lanes(0)],
                                            x_s.at[ICI - 2 + h], x_r.at[ICI - 2 + h], device_id={'tensor': xnb})

    def y_pair(h):
        return pltpu.make_async_remote_copy(gi.at[pl.ds(2, 2), row_half[h], lanes(0)], gi.at[pair, row_half[h], lanes(1)],
                                            y_s.at[ICI - 2 + h], y_r.at[ICI - 2 + h], device_id={'tensor': ynb})

    def mate_pair(h):
        return pltpu.make_async_remote_copy(gi.at[pair, row_half[h]], gm.at[pl.ds(RING - 2, 2), row_half[h]],
                                            p_s.at[ICI - 2 + h], p_r.at[ICI - 2 + h], device_id={'tensor': mate})

    def mate_low(k):
        return pltpu.make_async_remote_copy(gi.at[ICI - 2 + k, row_half[1]], gm.at[RING - 2 + k, row_half[1]],
                                            p_s.at[ICI - 1 + k], p_r.at[ICI - 1 + k], device_id={'tensor': mate})

    def mate_copy(i):
        return pltpu.make_async_remote_copy(gi.at[i], gm.at[i % RING], p_s.at[i], p_r.at[i], device_id={'tensor': mate})

    for n in range(EARLY):
        send_own(n)
    for h in range(2):
        own_send(h).start()
    l_load.start()
    r_loads[1].start()

    def transpose(k, _):
        rows = pl.ds(pl.multiple_of(k * CW, CW), CW)
        for h in range(2):
            gt[lanes(h, GW), rows] = gl[h, rows, :].T
        dd[rows, :] = jnp.zeros((CW, N), F32)
        return 0

    lax.fori_loop(0, N // CW, transpose, 0)

    def x_part(halves, slot):
        for n in range(N // TW):
            cols = lanes(n, TW)
            part = sum(dot(a[...], rr[slot, cols, lanes(h, TW)], NT) for h, a in enumerate(halves))
            dd[:, cols] = dd[:, cols] + part

    def r_part(a, where):
        part = (1.0 - EMA_DECAY) * dot(gt[...], a[...], NN)
        for j, (b, c) in enumerate(where):
            cols = pl.ds(pl.multiple_of(c * CW, CW), CW)
            rn[b, :, cols] = EMA_DECAY * rn[b, :, cols] + part[:, j * CW:(j + 1) * CW]

    def l_part(halves, rows):
        for n in range(N // TW):
            cols = lanes(n, TW)
            part = sum(dot(a[rows, :], a[cols, :], NT) for a in halves)
            ln[rows, cols] = ln[rows, cols] + (1.0 - EMA_DECAY) * part

    l_load.wait()

    def decay(k, _):
        rows = pl.ds(pl.multiple_of(core * GW + k * 64, 64), 64)
        ln[rows, :] = EMA_DECAY * ln[rows, :]
        return 0

    lax.fori_loop(0, GW // 64, decay, 0)
    r_loads[0].wait()

    def arrive(i):
        x_copy(i, gi.at[i, :, lanes(0)]).wait_recv()
        y_copy(i, gi.at[i, :, lanes(1)]).wait_recv()
        if isinstance(i, int) and i < RING:
            mate_copy(i).start()
            return

        @pl.when(i >= RING)
        def _():
            pl.semaphore_wait(credit, 1)

        mate_copy(i).start()

    def arrive_pair(h):
        x_pair(h).wait_recv()
        y_pair(h).wait_recv()
        if h == 0:
            mate_pair(0).start()
        else:
            for k in range(2):
                mate_low(k).start()

    def issue(i):
        @pl.when(i < 8 - EARLY)
        def _():
            send_own(i + EARLY)

        @pl.when((i >= 8 - EARLY) & (i < ICI - 2 - EARLY))
        def _():
            send_forward(i + EARLY - 8)

        for h in range(2):
            @pl.when(i == ICI - 2 - EARLY + h)
            def _():
                x_pair(h).start()
                y_pair(h).start()

    def local_step(g, _):
        slot = g % 2
        where = local_pieces(g)
        halves = [gl.at[g, :, lanes(h, TW)] for h in range(2)]

        @pl.when(g < 3)
        def _():
            for c in rr_loads(local_pieces(g + 1), 1 - slot):
                c.start()

        @pl.when(g == 3)
        def _():
            for c in rr_loads(pieces(4), 0):
                c.start()

        @pl.when(g >= 2)
        def _():
            own_send(g - 2).wait()

        @pl.when(g == 1)
        def _():
            for c in r_loads[2:4]:
                c.start()

        @pl.when(g == 2)
        def _():
            r_loads[1].wait()
            for c in r_loads[4:6]:
                c.start()

        for c in rr_loads(where, slot):
            c.wait()
        x_part(halves, slot)
        r_part(halves[0], where[:2])

        @pl.when(g == 3)
        def _():
            arrive(0)
            issue(0)
            for c in r_loads[2:6]:
                c.wait()

        r_part(halves[1], where[2:])
        l_part(halves, half)
        return 0

    lax.fori_loop(0, 4, local_step, 0)
    v_load.start()
    r_loads[6].start()

    lr_loads = [pltpu.make_async_copy(lr_hbm.at[:, h * GW:(h + 1) * GW], gl.at[h], lr_sem.at[h]) for h in range(2)]

    def step(i, _):
        slot = i % 2
        where = pieces(4 + i)
        halves = [gi.at[i], gm.at[i % RING]]
        for c in rr_loads(pieces(5 + i), 1 - slot):
            c.start()

        mate_copy(i).wait_recv()
        for c in rr_loads(where, slot):
            c.wait()
        x_part(halves, slot)
        r_part(halves[0], where[:2])
        arrive(i + 1)
        issue(i + 1)
        r_part(halves[1], where[2:])
        l_part(halves, half)
        pl.semaphore_signal(credit, inc=1, device_id={'tensor': mate})
        return 0

    lax.fori_loop(0, 8, step, 0)

    def late_step(i, slot):
        for c in rr_loads(pieces(5 + i), 1 - slot):
            c.start()
        mate_copy(i).wait_recv()
        for c in rr_loads(pieces(4 + i), slot):
            c.wait()
        x_part([gi.at[i], gm.at[i % RING]], slot)

    late_step(8, 0)

    v_load.wait()

    def adam(k, total):
        rows = pl.ds(pl.multiple_of(k * 64, 64), 64)
        for h in range(2):
            grad = gl[h, rows, :].astype(F32)
            moment = EMA_DECAY * vn[rows, lanes(h, GW)] + (1.0 - EMA_DECAY) * grad * grad
            a = grad / (jnp.sqrt(moment) + ADAM_EPS)
            vn[rows, lanes(h, GW)] = moment
            total = total + jnp.sum(a * a, axis=0, keepdims=True)
        return total

    adam_sum = jnp.sum(lax.fori_loop(0, N // 64, adam, jnp.zeros((1, GW), F32)))

    arrive(jnp.int32(9))
    l_part([gi.at[8], gm.at[0]], half)
    for n in range(8):
        x_copy(n, own_chunk((n + 4) % 8)).wait_send()
        y_copy(n, own_chunk(n)).wait_send()
    for c in lr_loads:
        c.start()
    late_step(9, 1)
    for c in rr_loads(pieces(15), 1):
        c.start()
    pl.semaphore_wait(credit, 2)
    arrive_pair(0)
    l_part([gi.at[9], gm.at[1]], half)

    l_send = pltpu.make_async_remote_copy(ln.at[half, :], ln.at[half, :], own_s.at[2], own_r.at[2], device_id={'tensor': mate})
    l_send.start()

    for slot in range(2):
        for c in rr_loads(pieces(14 + slot), slot):
            c.wait()
    for c in lr_loads:
        c.wait()
    share = rn.at[NDEV - 1]

    def x_rows(rows, mine_too, mates_too, done, chunks=(0, 1)):
        for n in range(N // TW):
            cols = lanes(n, TW)
            value = dd[rows, cols]
            part = None
            for k in chunks:
                for take, a, at in ((mine_too, gi.at[ICI - 2 + k], 0), (mates_too, gm.at[RING - 2 + k], 1)):
                    if take:
                        term = dot(a[rows, :], rr[k, cols, lanes(at, TW)], NT)
                        part = term if part is None else part + term
            if done:
                gl[2 + n // 2, rows, lanes(n % 2, TW)] = (value + part).astype(BF16)
            else:
                dd[rows, cols] = value + part

    mate_pair(0).wait_recv()
    x_rows(row_half[0], True, True, True)
    for n in range(N // TW):
        share[:, lanes(n, TW)] = dot(gl[0], gl[2 + n // 2, row_half[0], lanes(n % 2, TW)], NN)
    arrive_pair(1)
    x_rows(row_half[1], True, False, False)
    mate_low(0).wait_recv()
    x_rows(row_half[1], False, True, False, (0,))
    mate_low(1).wait_recv()
    x_rows(row_half[1], False, True, True, (1,))
    total = jnp.zeros((1, TW), F32)
    for n in range(N // TW):
        cols = lanes(n, TW)
        part = share[:, cols] + dot(gl[1], gl[2 + n // 2, row_half[1], lanes(n % 2, TW)], NN)
        dd[:, cols] = part
        total = total + jnp.sum(part * part, axis=0, keepdims=True)
    mine[0] = jnp.full((8, CW), adam_sum, F32)
    mine[1] = jnp.full((8, CW), jnp.sum(total), F32)

    def norm_copy(k, slot_of, to):
        return pltpu.make_async_remote_copy(mine, sums.at[slot_of], n_s.at[k], n_r.at[k], device_id={'tensor': to})

    for k in range(1, NDEV):
        norm_copy(NDEV - 1 - k, NDEV - 1 - k, lax.rem(me + k, NDEV)).start()
    r_loads[NDEV - 1].start()
    l_send.wait()
    for k in range(1, NDEV):
        norm_copy(k - 1, k - 1, lax.rem(me + k, NDEV)).wait_recv()

    a_all = mine[0]
    d_all = mine[1]
    for k in range(NDEV - 1):
        a_all = a_all + sums[k, 0]
        d_all = d_all + sums[k, 1]
    ratio[...] = jnp.sqrt(a_all / d_all)

    for k in range(1, NDEV):
        norm_copy(NDEV - 1 - k, NDEV - 1 - k, lax.rem(me + k, NDEV)).wait_send()
    for j in range(2):
        x_copy(8 + j, gi.at[j, :, lanes(1)]).wait_send()
        y_copy(8 + j, gi.at[j, :, lanes(0)]).wait_send()
        x_pair(j).wait_send()
        y_pair(j).wait_send()
        mate_low(j).wait_send()
    mate_pair(0).wait_send()
    for i in range(ICI - 2):
        mate_copy(i).wait_send()
    for c in r_loads[6:]:
        c.wait()


def write_kernel(rn_in, dd_in, ln_in, vn, ratio, gi, gm, gt, l_out, r_out, d_out, v_out, rn, dd, ln, sem):
    me = lax.axis_index('tensor')
    to_mate = 1 - 2 * lax.rem(me, 2)
    xhop, yhop = 2 - 4 * lax.rem(lax.div(me, 2), 2), 4 - 8 * lax.div(me, 4)
    stores = []

    def store(src, dst):
        c = pltpu.make_async_copy(src, dst, sem.at[len(stores)])
        c.start()
        stores.append(c)

    def columns(b, c, w):
        dev = me + (b % 2) * to_mate + (b // 2 % 2) * xhop + (b // 4) * yhop
        return pl.ds(pl.multiple_of(dev * N + c * CW, CW), w)

    for b in range(6):
        store(rn_in.at[b], r_out.at[:, columns(b, 0, N)])
    store(vn, v_out)
    scale = ratio[0:1, 0:1]
    for n in range(N // TW):
        cols = pl.ds(n * TW, TW)
        dd[:, cols] = dd_in[:, cols] * scale
    store(dd, d_out)
    for b, slots in ((6, [gi.at[i] for i in range(8, ICI)]), (7, [gm.at[i % RING] for i in range(8, ICI)])):
        for c, a in enumerate(slots):
            part = (1.0 - EMA_DECAY) * dot(gt[...], a[...], NN)
            for j in range(2):
                cols = pl.ds((c + 4 * j) * CW, CW)
                rn[b, :, cols] = EMA_DECAY * rn_in[b, :, cols] + part[:, j * CW:(j + 1) * CW]
        store(rn.at[b], r_out.at[:, columns(b, 0, N)])
    halves = [gi.at[ICI - 2], gi.at[ICI - 1], gm.at[RING - 2], gm.at[RING - 1]]
    for n in range(N // TW):
        cols = pl.ds(n * TW, TW)
        part = sum(dot(a[...], a[cols, :], NT) for a in halves)
        ln[:, cols] = ln_in[:, cols] + (1.0 - EMA_DECAY) * part
    store(ln, l_out)
    for c in stores:
        c.wait()


def solution(mesh):
    col_spec = P('layer', 'tensor')
    rep_spec = P('layer', None)
    row_spec = P(('layer', 'tensor'), None)
    hbm = pl.BlockSpec(memory_space=pl.ANY)
    vmem = pl.BlockSpec(memory_space=pltpu.VMEM)
    dma = pltpu.SemaphoreType.DMA

    def local_step(grad_loc, left_stat, right_loc, left_root, root_loc, moment_loc):
        mids = pl.pallas_call(
            gather_kernel,
            name='gather_compute',
            out_shape=(pltpu.VMEM((NDEV, N, N), F32), pltpu.VMEM((N, N), F32), pltpu.VMEM((N, N), F32), pltpu.VMEM((N, N), F32), pltpu.VMEM((8, CW), F32),
                       pltpu.VMEM((ICI, N, TW), BF16), pltpu.VMEM((RING, N, TW), BF16), pltpu.VMEM((N, N), BF16)),
            in_specs=[hbm] * 6,
            out_specs=(vmem,) * 8,
            scratch_shapes=[
                pltpu.VMEM((4, N, GW), BF16),
                pltpu.VMEM((2, N, GW), BF16),
                pltpu.VMEM((2, 8, CW), F32),
                pltpu.VMEM((NDEV - 1, 2, 8, CW), F32),
                dma((4,)), dma((8,)), dma((2, 4)), dma((2,)),
                dma((3,)), dma((3,)), dma((ICI,)), dma((ICI,)), dma((ICI,)), dma((ICI,)),
                dma((ICI + 1,)), dma((ICI + 1,)), dma((NDEV - 1,)), dma((NDEV - 1,)), pltpu.SemaphoreType.REGULAR,
            ],
            compiler_params=pltpu.CompilerParams(collective_id=0, has_side_effects=True, vmem_limit_bytes=VM1),
            cost_estimate=pl.CostEstimate(flops=46 * 2**30, bytes_accessed=60 * 2**20, transcendentals=2**20),
        )(grad_loc, left_stat, right_loc, left_root, root_loc, moment_loc)
        left_new, right_new, direction, moment_new, _, _, _ = pl.pallas_call(
            write_kernel,
            name='write_results',
            out_shape=(jax.ShapeDtypeStruct((N, N), F32), jax.ShapeDtypeStruct((N, NDEV * N), F32),
                       jax.ShapeDtypeStruct((N, N), F32), jax.ShapeDtypeStruct((N, N), F32),
                       pltpu.VMEM((NDEV, N, N), F32), pltpu.VMEM((N, N), F32), pltpu.VMEM((N, N), F32)),
            in_specs=[vmem] * 8,
            out_specs=(hbm,) * 4 + (vmem,) * 3,
            input_output_aliases={0: 4, 1: 5, 2: 6},
            scratch_shapes=[dma((11,))],
            compiler_params=pltpu.CompilerParams(vmem_limit_bytes=VM2),
        )(*(pltpu.with_memory_space_constraint(t, pltpu.VMEM) for t in mids))
        return left_new, right_new, direction, moment_new

    return jax.shard_map(local_step, mesh=mesh, in_specs=(col_spec, rep_spec, row_spec, rep_spec, row_spec, col_spec),
                         out_specs=(rep_spec, row_spec, col_spec, col_spec), check_vma=False)


VM1 = 79 * 2**17
VM2 = VM1
```
